8 devices in a mesh: dp: 1 (over z), tp: 2 (over y), cp: 4 (over x, core).
Axes of the slice: x: 2, y: 2, z: 1, core: 2. Of those that a mesh axis runs over, the one named last changes fastest.
Arguments:
- hidden_in: bfloat16 [256, 2048], P(('dp', 'cp', 'tp'))
- positions: int32 [256], P(('dp', 'cp', 'tp'))
- cache_len: int32 [1], P('dp')
- cache_k: bfloat16 [32768, 256], P(('dp', 'cp', 'tp'))
- cache_v: bfloat16 [32768, 256], P(('dp', 'cp', 'tp'))
- norm1_gain: bfloat16 [2048], replicated
- w_query: bfloat16 [2048, 2048], P(None, 'tp')
- w_key: bfloat16 [2048, 256], P(None, 'tp')
- w_value: bfloat16 [2048, 256], P(None, 'tp')
- w_out: bfloat16 [2048, 2048], P('tp')
- norm2_gain: bfloat16 [2048], replicated
- w_gate: bfloat16 [2048, 11008], P(None, 'tp')
- w_up: bfloat16 [2048, 11008], P(None, 'tp')
- w_down: bfloat16 [11008, 2048], P('tp')
Outputs:
- output: bfloat16 [256, 2048], P(('dp', 'cp', 'tp'))
All inputs are finite; a program needn't handle non-finite values.
Results may differ from the reference program's by a relative error of at most 0.0110318.
Values are sent between devices in bfloat16 or wider.
A program may use at most 1 GiB of HBM per device.

```python
import math
import jax
import jax.numpy as jnp
from jax import lax

TOKENS = 256
PREFIX = 32768
D_MODEL = 2048
Q_HEADS = 16
KV_HEADS = 2
HEAD_DIM = 128
FFN_DIM = 11008
SHARD_COUNT = 8
SHARD_ROWS = 32
QUERY_BLOCK = 32
ROPE_BASE = 500000.0
NORM_EPS = 1e-5


def normal_draw(rand_key, out_shape, spread):
    return (jax.random.normal(rand_key, out_shape, jnp.float32) * spread).astype(jnp.bfloat16)


def setup_inputs(seed: int = 0, part: int = 0) -> dict:
    base_key = jax.random.key(seed)
    part_keys = jax.random.split(jax.random.fold_in(base_key, part), 4)
    shared_keys = jax.random.split(jax.random.key(seed + 1), 9)
    cache_len = jax.random.randint(part_keys[0], (1,), PREFIX // 16, PREFIX + 1, dtype=jnp.int32)
    row_ids = jnp.arange(TOKENS, dtype=jnp.int32)
    half_rows = SHARD_ROWS // 2
    shard_ids = row_ids // SHARD_ROWS
    within = row_ids % SHARD_ROWS
    segment = jnp.where(within < half_rows, shard_ids, 2 * SHARD_COUNT - 1 - shard_ids)
    positions = cache_len[0] + segment * half_rows + within % half_rows
    qk_std = math.log((PREFIX + TOKENS) / 4.0) ** 0.25
    width_std = D_MODEL ** -0.5
    kv_width = KV_HEADS * HEAD_DIM
    return {
        'hidden_in': normal_draw(part_keys[1], (TOKENS, D_MODEL), 1.0),
        'positions': positions,
        'cache_len': cache_len,
        'cache_k': normal_draw(part_keys[2], (PREFIX, kv_width), qk_std),
        'cache_v': normal_draw(part_keys[3], (PREFIX, kv_width), 1.0),
        'norm1_gain': (1.0 + 0.3 * jax.random.normal(shared_keys[0], (D_MODEL,), jnp.float32)).astype(jnp.bfloat16),
        'w_query': normal_draw(shared_keys[1], (D_MODEL, Q_HEADS * HEAD_DIM), qk_std * width_std),
        'w_key': normal_draw(shared_keys[2], (D_MODEL, kv_width), qk_std * width_std),
        'w_value': normal_draw(shared_keys[3], (D_MODEL, kv_width), width_std),
        'w_out': normal_draw(shared_keys[4], (Q_HEADS * HEAD_DIM, D_MODEL), 2.0 * (Q_HEADS * HEAD_DIM) ** -0.5),
        'norm2_gain': (1.0 + 0.3 * jax.random.normal(shared_keys[5], (D_MODEL,), jnp.float32)).astype(jnp.bfloat16),
        'w_gate': normal_draw(shared_keys[6], (D_MODEL, FFN_DIM), width_std),
        'w_up': normal_draw(shared_keys[7], (D_MODEL, FFN_DIM), width_std),
        'w_down': normal_draw(shared_keys[8], (FFN_DIM, D_MODEL), FFN_DIM ** -0.5),
    }


def rms_norm(hidden, norm_gain):
    values = hidden.astype(jnp.float32)
    inv_rms = lax.rsqrt(jnp.mean(values * values, axis=-1, keepdims=True) + NORM_EPS)
    return (values * inv_rms * norm_gain.astype(jnp.float32)).astype(jnp.bfloat16)


def rotary(projected, positions):
    half_dim = HEAD_DIM // 2
    inv_freq = 1.0 / (ROPE_BASE ** (jnp.arange(half_dim, dtype=jnp.float32) * (2.0 / HEAD_DIM)))
    angles = positions.astype(jnp.float32)[:, None] * inv_freq[None, :]
    expand = (angles.shape[0],) + (1,) * (projected.ndim - 2) + (half_dim,)
    cos_table = jnp.cos(angles).reshape(expand)
    sin_table = jnp.sin(angles).reshape(expand)
    first_half = projected[..., :half_dim]
    second_half = projected[..., half_dim:]
    rotated = jnp.concatenate([first_half * cos_table - second_half * sin_table, second_half * cos_table + first_half * sin_table], axis=-1)
    return rotated.astype(jnp.bfloat16)


def reference(hidden_in, positions, cache_len, cache_k, cache_v, norm1_gain, w_query, w_key, w_value, w_out, norm2_gain, w_gate, w_up, w_down):
    groups = Q_HEADS // KV_HEADS
    block_count = TOKENS // QUERY_BLOCK
    score_scale = 1.0 / math.sqrt(HEAD_DIM)
    normed = rms_norm(hidden_in, norm1_gain)
    queries = rotary(jnp.dot(normed, w_query, preferred_element_type=jnp.float32).reshape(TOKENS, KV_HEADS, groups, HEAD_DIM), positions)
    new_keys = rotary(jnp.dot(normed, w_key, preferred_element_type=jnp.float32).reshape(TOKENS, KV_HEADS, HEAD_DIM), positions)
    new_values = jnp.dot(normed, w_value, preferred_element_type=jnp.float32).astype(jnp.bfloat16).reshape(TOKENS, KV_HEADS, HEAD_DIM)
    head_keys = jnp.moveaxis(new_keys, 1, 0)
    head_values = jnp.moveaxis(new_values, 1, 0)
    cached_keys = jnp.moveaxis(cache_k.reshape(PREFIX, KV_HEADS, HEAD_DIM), 1, 0)
    cached_values = jnp.moveaxis(cache_v.reshape(PREFIX, KV_HEADS, HEAD_DIM), 1, 0)
    cache_valid = jnp.arange(PREFIX) < cache_len[0]
    query_blocks = jnp.moveaxis(queries.reshape(block_count, QUERY_BLOCK, KV_HEADS, groups, HEAD_DIM), 2, 1)
    position_blocks = positions.reshape(block_count, QUERY_BLOCK)

    def attend_block(block_item):
        block_queries, block_pos = block_item
        causal = positions[None, None, :] <= block_pos[None, :, None]

        def attend_head(head_item):
            head_queries, cache_key_head, cache_value_head, new_key_head, new_value_head = head_item
            query_wide = head_queries.astype(jnp.float32)
            cache_scores = jnp.einsum('rgd,sd->grs', query_wide, cache_key_head.astype(jnp.float32)) * score_scale
            new_scores = jnp.einsum('rgd,sd->grs', query_wide, new_key_head.astype(jnp.float32)) * score_scale
            cache_scores = jnp.where(cache_valid[None, None, :], cache_scores, -jnp.inf)
            new_scores = jnp.where(causal, new_scores, -jnp.inf)
            row_max = jnp.maximum(jnp.max(cache_scores, axis=-1, keepdims=True), jnp.max(new_scores, axis=-1, keepdims=True))
            cache_probs = jnp.exp(cache_scores - row_max)
            new_probs = jnp.exp(new_scores - row_max)
            normalizer = jnp.sum(cache_probs, axis=-1, keepdims=True) + jnp.sum(new_probs, axis=-1, keepdims=True)
            weighted = jnp.einsum('grs,sd->grd', cache_probs.astype(jnp.bfloat16).astype(jnp.float32), cache_value_head.astype(jnp.float32))
            weighted = weighted + jnp.einsum('grs,sd->grd', new_probs.astype(jnp.bfloat16).astype(jnp.float32), new_value_head.astype(jnp.float32))
            return (weighted / normalizer).astype(jnp.bfloat16)

        return lax.map(attend_head, (block_queries, cached_keys, cached_values, head_keys, head_values))

    attended = lax.map(attend_block, (query_blocks, position_blocks))
    attended = jnp.transpose(attended, (0, 3, 1, 2, 4)).reshape(TOKENS, Q_HEADS * HEAD_DIM)
    residual_mid = (hidden_in.astype(jnp.float32) + jnp.dot(attended, w_out, preferred_element_type=jnp.float32)).astype(jnp.bfloat16)
    normed_mid = rms_norm(residual_mid, norm2_gain)
    gate_proj = jnp.dot(normed_mid, w_gate, preferred_element_type=jnp.float32)
    up_proj = jnp.dot(normed_mid, w_up, preferred_element_type=jnp.float32)
    hidden_mlp = (jax.nn.silu(gate_proj) * up_proj).astype(jnp.bfloat16)
    return (residual_mid.astype(jnp.float32) + jnp.dot(hidden_mlp, w_down, preferred_element_type=jnp.float32)).astype(jnp.bfloat16)
```

```python
import functools
import math

import jax
import jax.numpy as jnp
from jax import lax
from jax.experimental import pallas as pl
from jax.experimental.pallas import tpu as pltpu
from jax.sharding import PartitionSpec as P

HEAD_DIM = 128
ROPE_BASE = 500000.0
NORM_EPS = 1e-5
MESH = pl.DeviceIdType.MESH
F32 = jnp.float32
BF16 = jnp.bfloat16

ROWS = 32
D = 2048
HEADS = 8
SLOTS = 8192
HALF = 4096
QT = ROWS * HEADS
CS = 1024
NCH = SLOTS // CS
SUB = 256
FCOLS = 2816
NEG = -(2.0 ** 100)
SCALE = math.log2(math.e) / math.sqrt(HEAD_DIM)
OROWS = HEAD_DIM + 8


def rel_position(index):
    dev, row = lax.div(index, ROWS), lax.rem(index, ROWS)
    half = ROWS // 2
    seg = jnp.where(row < half, dev, 15 - dev)
    return seg * half + lax.rem(row, half)


def rms(values, gain):
    inv = lax.rsqrt(jnp.mean(values * values, axis=-1, keepdims=True) + NORM_EPS)
    return (values * inv * gain).astype(BF16)


def kernel(len_ref, x_ref, cos_ref, sin_ref, g1_ref, g2_ref, ck_ref, cv_ref, wq_hbm, wk_hbm, wv_hbm, wo_hbm, wg_hbm, wu_hbm, wd_hbm,
           out_ref,
           wq, wk, wv, wo, wg, wu, wd, kbuf, vbuf, vt, bias, abuf, qown, qbuf, kvbuf, s0, s1, obuf, land, newo, hbuf, aout, asend, arecv,
           bbuf, ubuf, dsend, drecv, down, ysend, yrecv,
           ld_sem, cs_sem, cr_sem, a_sem, qs_sem, qr_sem, kvs_sem, kvr_sem, os_sem, or_sem, w_sem, bs_sem, br_sem,
           ds_sem, dr_sem, ys_sem, yr_sem):
    c = lax.axis_index('cp')
    t = lax.axis_index('tp')
    x, k = lax.div(c, 2), lax.rem(c, 2)
    xo, ko, to = 1 - x, 1 - k, 1 - t
    partner = {'cp': x * 2 + ko, 'tp': t}
    ynbr = {'cp': c, 'tp': to}
    is_worker = k == t

    def remote(src, dst, ssem, rsem, dev):
        return pltpu.make_async_remote_copy(src_ref=src, dst_ref=dst, send_sem=ssem, recv_sem=rsem, device_id=dev, device_id_type=MESH)

    barrier = pltpu.get_barrier_semaphore()
    for dc in range(4):
        for dt in range(2):
            if dc or dt:
                pl.semaphore_signal(barrier, inc=1, device_id={'cp': lax.rem(c + dc, 4), 'tp': lax.rem(t + dt, 2)}, device_id_type=MESH)

    def local(src, dst, i):
        return pltpu.make_async_copy(src, dst, ld_sem.at[i])

    kcol = pl.multiple_of(k * HEAD_DIM, HEAD_DIM)
    kocol = pl.multiple_of(ko * HEAD_DIM, HEAD_DIM)
    myhalf = pl.multiple_of(k * HALF, HALF)
    fcol = pl.multiple_of(k * (5504 - FCOLS), 128)
    l_wq = local(wq_hbm, wq, 0)
    l_wk = local(wk_hbm, wk, 1)
    l_wv = local(wv_hbm, wv, 2)
    l_k = local(ck_ref.at[:, pl.ds(kcol, HEAD_DIM)], kbuf.at[pl.ds(myhalf, HALF), :], 3)
    l_v = local(cv_ref.at[:, pl.ds(kcol, HEAD_DIM)], vbuf.at[pl.ds(myhalf, HALF), :], 4)
    l_wo = local(wo_hbm, wo, 5)
    l_wg = local(wg_hbm.at[:, pl.ds(fcol, FCOLS)], wg, 6)
    l_wu = local(wu_hbm.at[:, pl.ds(fcol, FCOLS)], wu, 7)
    l_wd = local(wd_hbm.at[pl.ds(fcol, FCOLS), :], wd, 8)
    for copy in (l_wq, l_wk, l_wv, l_v, l_k):
        copy.start()

    g1 = g1_ref[...].astype(F32)
    myrow = pl.multiple_of(t * ROWS, ROWS)
    abuf[pl.ds(myrow, ROWS), :] = rms(x_ref[...].astype(F32), g1)

    pl.semaphore_wait(barrier, 7)
    a_copy = remote(abuf.at[pl.ds(myrow, ROWS), :], abuf.at[pl.ds(myrow, ROWS), :], a_sem.at[0], a_sem.at[1], ynbr)
    a_copy.start()
    r_v = remote(cv_ref.at[:, pl.ds(kocol, HEAD_DIM)], vbuf.at[pl.ds(myhalf, HALF), :], cs_sem.at[0], cr_sem.at[0], partner)
    r_k = remote(ck_ref.at[:, pl.ds(kocol, HEAD_DIM)], kbuf.at[pl.ds(myhalf, HALF), :], cs_sem.at[1], cr_sem.at[1], partner)
    r_v.start()
    r_k.start()

    clen = len_ref[0]
    lane0 = lax.broadcasted_iota(jnp.int32, (SUB, HEAD_DIM), 1) == 0
    rowi = lax.broadcasted_iota(jnp.int32, (SUB, HEAD_DIM), 0)

    def bias_body(i, _):
        part = lax.div(i, HALF // SUB)
        base = HALF * (4 * x + 2 * part + t) + lax.rem(i, HALF // SUB) * SUB
        hidden = (rowi + base >= clen) & lane0
        bias[pl.ds(pl.multiple_of(i * SUB, SUB), SUB), :] = jnp.where(hidden, NEG, 0.0).astype(BF16)
        return 0

    lax.fori_loop(0, SLOTS // SUB, bias_body, 0)

    eye = (lax.broadcasted_iota(jnp.int32, (HEAD_DIM, HEAD_DIM), 0) == lax.broadcasted_iota(jnp.int32, (HEAD_DIM, HEAD_DIM), 1)).astype(F32).astype(BF16)

    def transpose_half(base):
        def body(i, _):
            off = pl.multiple_of(base + i * 512, 512)
            vals = vbuf[pl.ds(off, 512), :]
            vt[:, pl.ds(off, 512)] = lax.dot_general(eye, vals, (((1,), (1,)), ((), ())), preferred_element_type=F32).astype(BF16)
            return 0
        lax.fori_loop(0, HALF // 512, body, 0)

    l_v.wait()
    transpose_half(myhalf)

    l_wq.wait()
    l_wk.wait()
    l_wv.wait()
    for copy in (l_wo, l_wg, l_wu, l_wd):
        copy.start()
    a_copy.wait()
    acts = abuf[...]
    cos, sin = cos_ref[...], sin_ref[...]

    def rope(vals):
        return (vals * cos + pltpu.roll(vals, HEAD_DIM // 2, 1) * sin).astype(BF16)

    for hp in range(HEADS // 2):
        prod = jnp.dot(acts, wq[:, hp * 256:(hp + 1) * 256], preferred_element_type=F32)
        for sub in range(2):
            h = hp * 2 + sub
            rot = rope(prod[:, sub * HEAD_DIM:(sub + 1) * HEAD_DIM])
            qown[0, h * ROWS:(h + 1) * ROWS, :] = rot[:ROWS]
            qown[1, h * ROWS:(h + 1) * ROWS, :] = rot[ROWS:]

    def q_copy(dx, dy, ph):
        j = to if ph == 0 else t
        dev = {'cp': lax.rem(x + dx, 2) * 2 + t, 'tp': lax.rem(t + dy, 2)}
        n = (dx * 2 + dy) * 2 + ph
        return remote(qown.at[j], qbuf.at[c, j], qs_sem.at[n], qr_sem.at[c, j], dev)

    for ph in range(2):
        for dx, dy in ((0, 1), (0, 0), (1, 0), (1, 1)):
            if dx or dy:
                q_copy(dx, dy, ph).start()
            else:
                @pl.when(jnp.logical_not(is_worker))
                def _():
                    q_copy(0, 0, ph).start()

    @pl.when(is_worker)
    def _():
        qbuf[c] = qown[...]

    kvbuf[c, 0] = rope(jnp.dot(acts, wk[...], preferred_element_type=F32))
    kvbuf[c, 1] = jnp.dot(acts, wv[...], preferred_element_type=F32).astype(BF16)

    def kv_copy(dc):
        return remote(kvbuf.at[c], kvbuf.at[c], kvs_sem.at[dc], kvr_sem.at[c], {'cp': lax.rem(c + dc, 4), 'tp': t})

    for dc in range(1, 4):
        kv_copy(dc).start()

    cr_half = pl.multiple_of(ko * HALF, HALF)
    r_v.wait_recv()
    transpose_half(cr_half)
    l_k.wait()
    r_k.wait_recv()

    one_col = (lax.broadcasted_iota(jnp.int32, (QT, HEAD_DIM), 1) == 0).astype(F32).astype(BF16)

    def merge(ph):
        for dw in range(4):
            wx, wy = dw // 2, dw % 2
            slot = lax.rem(x + wx, 2) * 2 + lax.rem(t + wy, 2)
            recv = remote(obuf.at[0], land.at[ph, slot], os_sem.at[0], or_sem.at[ph, slot], ynbr)
            if dw == 0:
                @pl.when(jnp.logical_not(is_worker))
                def _():
                    recv.wait_recv()
            else:
                recv.wait_recv()
        parts = [land[ph, w] for w in range(4)] + [newo[ph]]
        tops = [p[HEAD_DIM:HEAD_DIM + 1] for p in parts]
        top = functools.reduce(jnp.maximum, tops)
        scales = [jnp.exp2((m - top) * SCALE) for m in tops]
        total = sum(s * p[HEAD_DIM + 1:HEAD_DIM + 2] for s, p in zip(scales, parts))
        mixed = sum(s * p[:HEAD_DIM] for s, p in zip(scales, parts)) / total
        turned = mixed.T.astype(BF16)
        for h in range(HEADS):
            aout[:, h * HEAD_DIM:(h + 1) * HEAD_DIM] = turned[h * ROWS:(h + 1) * ROWS]
        return aout[...]

    def out_product(ph, store):
        vals = merge(ph)

        def body(i, _):
            cols = pl.ds(pl.multiple_of(i * 512, 512), 512)
            store(cols, jnp.dot(vals, wo[:, cols], preferred_element_type=F32))
            return 0
        lax.fori_loop(0, D // 512, body, 0)

    w_copy = remote(asend, arecv, w_sem.at[0], w_sem.at[1], ynbr)

    def new_rows():
        for dc in range(1, 4):
            src = lax.rem(c + dc, 4)
            remote(kvbuf.at[src], kvbuf.at[src], kvs_sem.at[0], kvr_sem.at[src], ynbr).wait_recv()
        keys = jnp.concatenate([kvbuf[b, 0] for b in range(4)], axis=0)
        vals = jnp.concatenate([kvbuf[b, 1] for b in range(4)], axis=0)
        key_pos = rel_position(lax.broadcasted_iota(jnp.int32, (256, QT), 0))
        lane = lax.rem(lax.broadcasted_iota(jnp.int32, (256, QT), 1), ROWS)
        for ph in range(2):
            j = to if ph == 0 else t
            scores = lax.dot_general(keys, qown[j], (((1,), (1,)), ((), ())), preferred_element_type=F32)
            scores = jnp.where(key_pos <= rel_position((c * 2 + j) * ROWS + lane), scores, NEG)
            top = jnp.max(scores, axis=0, keepdims=True)
            probs = jnp.exp2((scores - top) * SCALE)
            newo[ph, :HEAD_DIM, :] = lax.dot_general(vals, probs.astype(BF16), (((0,), (0,)), ((), ())), preferred_element_type=F32)
            newo[ph, HEAD_DIM:HEAD_DIM + 1, :] = top
            newo[ph, HEAD_DIM + 1:HEAD_DIM + 2, :] = jnp.sum(probs, axis=0, keepdims=True)

    def tile_place(n):
        ph, i = lax.div(n, 4), lax.rem(n, 4)
        flip = lax.rem(ph + lax.div(i, 2), 2)
        dk = lax.rem(ph + i, 2)
        blk = lax.rem(x + flip, 2) * 2 + lax.rem(k + dk, 2)
        j = lax.rem(k + 1 + ph, 2)
        return ph, blk, j

    def o_copy(n):
        ph, blk, _ = tile_place(n)
        slot = x * 2 + t
        return remote(obuf.at[n], land.at[ph, slot], os_sem.at[n], or_sem.at[ph, slot], {'cp': blk, 'tp': k})

    def scores_of(qa, ci, s_ref):
        top = None
        for sub in range(CS // SUB):
            rows = pl.ds(pl.multiple_of(ci * CS + sub * SUB, SUB), SUB)
            ka = jnp.concatenate([kbuf[rows, :], bias[rows, :]], axis=1)
            s = lax.dot_general(ka, qa, (((1,), (1,)), ((), ())), preferred_element_type=F32)
            s_ref[sub * SUB:(sub + 1) * SUB, :] = s
            mx = jnp.max(s.reshape(SUB // 8, 8, QT), axis=0)
            top = mx if top is None else jnp.maximum(top, mx)
        return jnp.max(top, axis=0, keepdims=True)

    def absorb(ci, s_ref, m_new, m, l, o):
        alpha = jnp.exp2((m - m_new) * SCALE)
        l = l * alpha
        acc = None
        for sub in range(CS // SUB):
            p = jnp.exp2((s_ref[sub * SUB:(sub + 1) * SUB, :] - m_new) * SCALE)
            l = l + jnp.sum(p.reshape(SUB // 8, 8, QT), axis=0)
            cols = pl.ds(pl.multiple_of(ci * CS + sub * SUB, SUB), SUB)
            part = jnp.dot(vt[:, cols], p.astype(BF16), preferred_element_type=F32)
            acc = part if acc is None else acc + part
        return l, o * alpha + acc

    def tile_body(n, _):
        ph, blk, j = tile_place(n)
        mine = jnp.logical_and(is_worker, blk == c)

        @pl.when(jnp.logical_not(mine))
        def _():
            remote(qown.at[j], qbuf.at[blk, j], qs_sem.at[0], qr_sem.at[blk, j], ynbr).wait_recv()

        @pl.when(n == 6)
        def _():
            new_rows()
            l_wo.wait()

            def store(cols, vals):
                asend[:, cols] = vals
            out_product(0, store)
            w_copy.start()

        qa = jnp.concatenate([qbuf[blk, j], one_col], axis=1)
        m0 = scores_of(qa, 0, s0)
        m = m0
        l = jnp.zeros((8, QT), F32)
        o = jnp.zeros((HEAD_DIM, QT), F32)

        def pair(i, carry):
            m, m0, l, o = carry
            m1 = jnp.maximum(m0, scores_of(qa, 2 * i + 1, s1))
            l, o = absorb(2 * i, s0, m0, m, l, o)
            nxt = jnp.minimum(2 * i + 2, NCH - 1)
            m2 = jnp.maximum(m1, scores_of(qa, nxt, s0))
            l, o = absorb(2 * i + 1, s1, m1, m0, l, o)
            return m1, m2, l, o

        m, _, l, o = lax.fori_loop(0, NCH // 2, pair, (m, m0, l, o))
        obuf[n, :HEAD_DIM, :] = o
        obuf[n, HEAD_DIM:HEAD_DIM + 1, :] = m
        obuf[n, HEAD_DIM + 1:HEAD_DIM + 2, :] = jnp.sum(l, axis=0, keepdims=True)

        @pl.when(jnp.logical_not(mine))
        def _():
            o_copy(n).start()

        @pl.when(mine)
        def _():
            land[ph, x * 2 + t] = obuf[n]
        return 0

    lax.fori_loop(0, 8, tile_body, 0)

    def store_mid(cols, vals):
        hbuf[:, cols] = vals
    out_product(1, store_mid)
    w_copy.wait_recv()
    mid = (x_ref[...].astype(F32) + (hbuf[...] + arecv[...])).astype(BF16)
    hbuf[...] = mid.astype(F32)

    place = pl.multiple_of((k * 2 + t) * ROWS, ROWS)
    bbuf[pl.ds(place, ROWS), :] = rms(mid.astype(F32), g2_ref[...].astype(F32))
    hr = ROWS // 2

    def b_copy(kind, i):
        if kind == 0:
            rows, dev = pl.multiple_of(place + i * hr, hr), ynbr
        elif kind == 1:
            rows, dev = pl.multiple_of(place + i * hr, hr), partner
        else:
            rows, dev = pl.multiple_of((k * 2 + to) * ROWS + i * hr, hr), partner
        piece = bbuf.at[pl.ds(rows, hr), :]
        return remote(piece, piece, bs_sem.at[kind, i], br_sem.at[kind, i], dev)

    for kind in (0, 1):
        for i in range(2):
            b_copy(kind, i).start()
    for i in range(2):
        b_copy(0, i).wait_recv()
        b_copy(2, i).start()
    l_wg.wait()
    l_wu.wait()
    for i in range(2):
        b_copy(1, i).wait_recv()
    for i in range(2):
        b_copy(2, i).wait_recv()

    def mlp_body(i, _):
        cols = pl.ds(pl.multiple_of(i * 256, 256), 256)
        acts2 = bbuf[...]
        gate = jnp.dot(acts2, wg[:, cols], preferred_element_type=F32)
        up = jnp.dot(acts2, wu[:, cols], preferred_element_type=F32)
        vals = gate / (1.0 + jnp.exp(-gate)) * up
        col = lax.broadcasted_iota(jnp.int32, (4 * ROWS, 256), 1) + i * 256
        keep = col >= k * (2 * FCOLS - 5504)
        ubuf[:, cols] = jnp.where(keep, vals, 0.0).astype(BF16)
        return 0

    lax.fori_loop(0, FCOLS // 256, mlp_body, 0)
    l_wd.wait()

    def d_copy(n):
        return remote(dsend.at[n], drecv.at[n], ds_sem.at[n], dr_sem.at[n], partner)

    def y_copy(n):
        return remote(ysend.at[n], yrecv.at[n], ys_sem.at[n], yr_sem.at[n], ynbr)

    keep_rows = pl.multiple_of(k * 64, 64)
    give_rows = pl.multiple_of(ko * 64, 64)

    def pass_on(n):
        d_copy(n).wait_recv()
        ysend[n] = down[n, pl.ds(keep_rows + pl.multiple_of(to * ROWS, ROWS), ROWS), :] + drecv[n, pl.ds(pl.multiple_of(to * ROWS, ROWS), ROWS), :]
        y_copy(n).start()

    lag = 4
    nblk = D // 256
    for n in range(nblk + lag):
        if n < nblk:
            down[n] = jnp.dot(ubuf[...], wd[:, n * 256:(n + 1) * 256], preferred_element_type=F32)
            dsend[n] = down[n, pl.ds(give_rows, 64), :]
            d_copy(n).start()
        if n >= lag:
            pass_on(n - lag)
    for n in range(nblk):
        y_copy(n).wait_recv()
        own = down[n, pl.ds(keep_rows + myrow, ROWS), :] + drecv[n, pl.ds(myrow, ROWS), :]
        cols = slice(n * 256, (n + 1) * 256)
        out_ref[:, cols] = (hbuf[:, cols] + (own + yrecv[n])).astype(BF16)

    r_v.wait_send()
    r_k.wait_send()
    for ph in range(2):
        for dx, dy in ((0, 1), (0, 0), (1, 0), (1, 1)):
            if dx or dy:
                q_copy(dx, dy, ph).wait_send()
            else:
                @pl.when(jnp.logical_not(is_worker))
                def _():
                    q_copy(0, 0, ph).wait_send()
    for dc in range(1, 4):
        kv_copy(dc).wait_send()

    def drain(n, _):
        _, blk, _ = tile_place(n)

        @pl.when(jnp.logical_not(jnp.logical_and(is_worker, blk == c)))
        def _():
            o_copy(n).wait_send()
        return 0

    lax.fori_loop(0, 8, drain, 0)
    w_copy.wait_send()
    for kind in range(3):
        for i in range(2):
            b_copy(kind, i).wait_send()
    for n in range(nblk):
        d_copy(n).wait_send()
        y_copy(n).wait_send()


def solution(mesh):
    token_spec = P(('dp', 'cp', 'tp'), None)
    column_spec = P(None, 'tp')
    row_spec = P('tp', None)

    def device_layer(hidden_loc, pos_loc, cache_len, cache_k, cache_v, norm1_gain, w_query, w_key, w_value, w_out, norm2_gain, w_gate, w_up, w_down):
        c = lax.axis_index('cp')
        pos = cache_len[0] + rel_position(c * 64 + jnp.arange(64, dtype=jnp.int32))
        half_dim = HEAD_DIM // 2
        inv_freq = 1.0 / (ROPE_BASE ** (jnp.arange(half_dim, dtype=F32) * (2.0 / HEAD_DIM)))
        angles = pos.astype(F32)[:, None] * inv_freq[None, :]
        cos, sin = jnp.cos(angles), jnp.sin(angles)
        cos2 = jnp.concatenate([cos, cos], axis=1)
        sin2 = jnp.concatenate([-sin, sin], axis=1)
        vmem = pl.BlockSpec(memory_space=pltpu.VMEM)
        hbm = pl.BlockSpec(memory_space=pl.ANY)
        dma = pltpu.SemaphoreType.DMA
        return pl.pallas_call(
            kernel,
            out_shape=jax.ShapeDtypeStruct((ROWS, D), BF16),
            in_specs=[pl.BlockSpec(memory_space=pltpu.SMEM)] + [vmem] * 5 + [hbm] * 9,
            out_specs=vmem,
            scratch_shapes=[
                pltpu.VMEM((D, 1024), BF16), pltpu.VMEM((D, 128), BF16), pltpu.VMEM((D, 128), BF16), pltpu.VMEM((1024, D), BF16),
                pltpu.VMEM((D, FCOLS), BF16), pltpu.VMEM((D, FCOLS), BF16), pltpu.VMEM((FCOLS, D), BF16),
                pltpu.VMEM((SLOTS, HEAD_DIM), BF16), pltpu.VMEM((SLOTS, HEAD_DIM), BF16), pltpu.VMEM((HEAD_DIM, SLOTS), BF16),
                pltpu.VMEM((SLOTS, HEAD_DIM), BF16),
                pltpu.VMEM((2 * ROWS, D), BF16), pltpu.VMEM((2, QT, HEAD_DIM), BF16), pltpu.VMEM((4, 2, QT, HEAD_DIM), BF16),
                pltpu.VMEM((4, 2, 64, HEAD_DIM), BF16),
                pltpu.VMEM((CS, QT), F32), pltpu.VMEM((CS, QT), F32),
                pltpu.VMEM((8, OROWS, QT), F32), pltpu.VMEM((2, 4, OROWS, QT), F32), pltpu.VMEM((2, OROWS, QT), F32),
                pltpu.VMEM((ROWS, D), F32), pltpu.VMEM((ROWS, 1024), BF16), pltpu.VMEM((ROWS, D), F32), pltpu.VMEM((ROWS, D), F32),
                pltpu.VMEM((4 * ROWS, D), BF16), pltpu.VMEM((4 * ROWS, FCOLS), BF16),
                pltpu.VMEM((8, 64, 256), F32), pltpu.VMEM((8, 64, 256), F32), pltpu.VMEM((8, 128, 256), F32),
                pltpu.VMEM((8, ROWS, 256), F32), pltpu.VMEM((8, ROWS, 256), F32),
                dma((9,)), dma((2,)), dma((2,)), dma((2,)), dma((8,)), dma((4, 2)), dma((4,)), dma((4,)), dma((8,)), dma((2, 4)), dma((2,)),
                dma((3, 2)), dma((3, 2)), dma((8,)), dma((8,)), dma((8,)), dma((8,)),
            ],
            compiler_params=pltpu.CompilerParams(collective_id=0, has_side_effects=True, vmem_limit_bytes=67043328),
            name='layer',
        )(cache_len, hidden_loc, cos2, sin2, norm1_gain.reshape(1, D), norm2_gain.reshape(1, D), cache_k, cache_v,
          w_query, w_key, w_value, w_out, w_gate, w_up, w_down)

    return jax.shard_map(device_layer, mesh=mesh, in_specs=(token_spec, P(('dp', 'cp', 'tp')), P('dp'), token_spec, token_spec, P(), column_spec, column_spec, column_spec, row_spec, P(), column_spec, column_spec, row_spec), out_specs=token_spec, check_vma=False)
```

```python
import functools
import math
import operator

import jax
import jax.numpy as jnp
from jax import lax
from jax.experimental import pallas as pl
from jax.experimental.pallas import tpu as pltpu
from jax.sharding import PartitionSpec as P

HEAD_DIM = 128
ROPE_BASE = 500000.0
NORM_EPS = 1e-5
MESH = pl.DeviceIdType.MESH
F32 = jnp.float32
BF16 = jnp.bfloat16

ROWS = 32
D = 2048
HEADS = 8
SLOTS = 8192
HALF = 4096
QT = ROWS * HEADS
CS = 1024
NCH = SLOTS // CS
VT = 512
ASIDE = 6
KC = 512
NC = 512
PART = 512
FCOLS = 2816
NEG = -(2.0 ** 100)
SCALE = math.log2(math.e) / math.sqrt(HEAD_DIM)
OROWS = HEAD_DIM + 8
PAIR = range(2)
OUT, TOP, NORM = (slice(*b) for b in ((0, HEAD_DIM), (HEAD_DIM, HEAD_DIM + 1), (HEAD_DIM + 1, HEAD_DIM + 2)))
CONTRACT_LAST = (((1,), (1,)), ((), ()))
PI_A = 201.0 / 128.0
PI_B = round((math.pi / 2 - PI_A) * 2.0 ** 20) / 2.0 ** 20
PI_C = math.pi / 2 - PI_A - PI_B


def rel_position(index):
    half = ROWS // 2
    dev, high = index >> 5, (index >> 4) & 1
    seg = dev + high * (15 - 2 * dev)
    return seg * half + (index & (half - 1))


def turn(angle):
    n = jnp.floor(angle * (2.0 / math.pi) + 0.5)
    r = ((angle - n * PI_A) - n * PI_B) - n * PI_C
    z = r * r
    sin = r + r * z * (-1.6666654611e-1 + z * (8.3321608736e-3 + z * -1.9515295891e-4))
    cos = 1.0 - 0.5 * z + z * z * (4.166664568298827e-2 + z * (-1.388731625493765e-3 + z * 2.443315711809948e-5))
    quarter = n - 4.0 * jnp.floor(n * 0.25)
    odd = (quarter == 1.0) | (quarter == 3.0)
    cos, sin = jnp.where(odd, sin, cos), jnp.where(odd, cos, sin)
    return jnp.where((quarter == 1.0) | (quarter == 2.0), -cos, cos), jnp.where(quarter >= 2.0, -sin, sin)


def par(first, *more):
    return lax.rem(sum(more, first), 2)


def over_rows(op, vals):
    return op(vals, axis=0, keepdims=True)


def block(i, size):
    return slice(i * size, (i + 1) * size)


def wide(gain_ref):
    gain = gain_ref[...].astype(F32)
    return jnp.concatenate([gain[i:i + 1] for i in range(D // 128)], axis=1)


def rms(values, gain):
    inv = lax.rsqrt(jnp.mean(values * values, axis=-1, keepdims=True) + NORM_EPS)
    return (values * inv * gain).astype(BF16)


def kernel(len_ref, x_hbm, freq_hbm, g1_hbm, g2_hbm, ck_ref, cv_ref, wq_hbm, wk_hbm, wv_hbm, wo_hbm, wg_hbm, wu_hbm, wd_hbm,
           out_hbm,
           x_ref, freq_ref, g1_ref, g2_ref, wq, wk, wv, wo, wg, wu, wd, kbuf, vbuf, vt, abuf, qown, qbuf, kvbuf, s0, s1, p0, p1, oacc, obuf, passing, land, newo, hbuf, asend, arecv,
           bbuf, ubuf, drecv, yrecv, out_ref,
           ld_sem, cs_sem, cr_sem, a_sem, qs_sem, qr_sem, kvs_sem, kvr_sem, os_sem, ps_sem, or_sem, ws_sem, wr_sem, bs_sem, br_sem,
           us_sem, ur_sem, ds_sem, dr_sem, ys_sem, yr_sem, out_sem):
    c = lax.axis_index('cp')
    t = lax.axis_index('tp')
    x, k = lax.div(c, 2), par(c)
    xo, ko, to = 1 - x, 1 - k, 1 - t
    partner = {'cp': x * 2 + ko, 'tp': t}
    ynbr = {'cp': c, 'tp': to}
    is_worker = k == t

    def remote(src, dst, ssem, rsem, dev):
        return pltpu.make_async_remote_copy(src_ref=src, dst_ref=dst, send_sem=ssem, recv_sem=rsem, device_id=dev, device_id_type=MESH)

    barrier = pltpu.get_barrier_semaphore()
    for dc in range(4):
        for dt in PAIR:
            if dc or dt:
                pl.semaphore_signal(barrier, inc=1, device_id={'cp': lax.rem(c + dc, 4), 'tp': par(t, dt)}, device_id_type=MESH)

    def local(src, dst, i):
        return pltpu.make_async_copy(src, dst, ld_sem.at[i])

    kcol = pl.multiple_of(k * HEAD_DIM, HEAD_DIM)
    kocol = pl.multiple_of(ko * HEAD_DIM, HEAD_DIM)
    myhalf = pl.multiple_of(k * HALF, HALF)
    fcol = pl.multiple_of(k * (5504 - FCOLS), 128)
    l_wq = local(wq_hbm, wq, 0)
    l_wk = local(wk_hbm, wk, 1)
    l_wv = local(wv_hbm, wv, 2)
    l_k = local(ck_ref.at[:, pl.ds(kcol, HEAD_DIM)], kbuf.at[pl.ds(myhalf, HALF), :], 3)
    l_v = local(cv_ref.at[:, pl.ds(kcol, HEAD_DIM)], vbuf.at[pl.ds(myhalf, HALF), :], 4)
    l_wo = local(wo_hbm, wo, 5)
    l_wg = local(wg_hbm.at[:, pl.ds(fcol, FCOLS)], wg, 6)
    l_wu = local(wu_hbm.at[:, pl.ds(fcol, FCOLS)], wu, 7)
    l_wd = local(wd_hbm.at[:, pl.ds(pl.multiple_of(k * (D // 2), 128), D // 2)], wd, 8)
    l_x = local(x_hbm, x_ref, 9)
    l_g1 = local(g1_hbm, g1_ref, 10)
    l_g2 = local(g2_hbm, g2_ref, 11)
    l_freq = local(freq_hbm, freq_ref, 12)
    for copy in (l_x, l_g1, l_wq, l_v, l_wk, l_wv, l_freq, l_k, l_g2):
        copy.start()

    l_x.wait()
    l_g1.wait()
    g1 = wide(g1_ref)
    myrow = pl.multiple_of(t * ROWS, ROWS)
    abuf[pl.ds(myrow, ROWS), :] = rms(x_ref[...].astype(F32), g1)

    pl.semaphore_wait(barrier, 7)
    a_copy = remote(abuf.at[pl.ds(myrow, ROWS), :], abuf.at[pl.ds(myrow, ROWS), :], a_sem.at[0], a_sem.at[1], ynbr)
    a_copy.start()
    r_v = remote(cv_ref.at[:, pl.ds(kocol, HEAD_DIM)], vbuf.at[pl.ds(myhalf, HALF), :], cs_sem.at[0], cr_sem.at[0], partner)
    r_k = remote(ck_ref.at[:, pl.ds(kocol, HEAD_DIM)], kbuf.at[pl.ds(myhalf, HALF), :], cs_sem.at[1], cr_sem.at[1], partner)
    r_v.start()
    r_k.start()

    clen = len_ref[0]
    rowi, lane = (lax.broadcasted_iota(jnp.int32, (VT, HEAD_DIM), i) for i in PAIR)
    lane0 = lane == 0
    eye = operator.eq(*(lax.broadcasted_iota(jnp.int32, (HEAD_DIM, HEAD_DIM), i) for i in PAIR)).astype(F32).astype(BF16)

    def turn_half(core):
        def body(i, _):
            off = pl.multiple_of(core * HALF + i * VT, VT)
            vals = vbuf[pl.ds(off, VT), :]
            vt[:, pl.ds(off, VT)] = lax.dot_general(eye, vals, CONTRACT_LAST, preferred_element_type=F32).astype(BF16)
            hidden = (rowi + (HALF * (4 * x + 2 * core + t) + i * VT) >= clen) & lane0
            vbuf[pl.ds(off, VT), :] = jnp.where(hidden, NEG, 0.0).astype(BF16)
            return 0
        lax.fori_loop(0, HALF // VT, body, 0)

    l_v.wait()
    turn_half(k)

    one_col = (lax.broadcasted_iota(jnp.int32, (QT, HEAD_DIM), 1) == 0).astype(F32).astype(BF16)
    for n in range(8):
        qbuf[n, :, HEAD_DIM:] = one_col
    l_freq.wait()
    pos = clen + rel_position(c * 64 + lax.broadcasted_iota(jnp.int32, (64, HEAD_DIM // 2), 0))
    cos, sin = turn(pos.astype(F32) * freq_ref[0:1, :])
    oacc[...] = jnp.zeros((HEAD_DIM, QT), F32)

    l_wq.wait()
    l_wk.wait()
    l_wv.wait()
    for copy in (l_wo, l_wg, l_wu, l_wd):
        copy.start()
    a_copy.wait()
    acts = abuf[...]
    cos = jnp.concatenate([cos, cos], axis=1)
    sin = jnp.concatenate([-sin, sin], axis=1)

    def rope(vals):
        return (vals * cos + pltpu.roll(vals, HEAD_DIM // 2, 1) * sin).astype(BF16)

    for hp in range(HEADS // 2):
        prod = jnp.dot(acts, wq[:, hp * 256:(hp + 1) * 256], preferred_element_type=F32)
        for sub in PAIR:
            h = hp * 2 + sub
            rot = rope(prod[:, sub * HEAD_DIM:(sub + 1) * HEAD_DIM])
            qown[0, h * ROWS:(h + 1) * ROWS, :] = rot[:ROWS]
            qown[1, h * ROWS:(h + 1) * ROWS, :] = rot[ROWS:]

    def q_copy(dx, dy, ph):
        j = to if ph == 0 else t
        dev = {'cp': par(x, dx) * 2 + t, 'tp': par(t, dy)}
        n = (dx * 2 + dy) * 2 + ph
        tile = ph * 4 + (dx + max(dy, ph)) % 2 * 2 + par(k, t, ph)
        return remote(qown.at[j], qbuf.at[tile, :, :HEAD_DIM], qs_sem.at[n], qr_sem.at[tile], dev)

    def send_queries(ph, places):
        for dx, dy in places:
            if dx or dy:
                q_copy(dx, dy, ph).start()
            else:
                @pl.when(jnp.logical_not(is_worker))
                def _():
                    q_copy(0, 0, ph).start()

    send_queries(0, ((1, 1), (0, 0)))

    @pl.when(is_worker)
    def _():
        qbuf[0, :, :HEAD_DIM] = qown[to]
        qbuf[7, :, :HEAD_DIM] = qown[t]

    kvbuf[c, 0] = rope(jnp.dot(acts, wk[...], preferred_element_type=F32))
    kvbuf[c, 1] = jnp.dot(acts, wv[...], preferred_element_type=F32).astype(BF16)

    def kv_copy(dc):
        return remote(kvbuf.at[c], kvbuf.at[c], kvs_sem.at[dc], kvr_sem.at[c], {'cp': lax.rem(c + dc, 4), 'tp': t})

    r_v.wait_recv()
    turn_half(ko)
    send_queries(0, ((0, 1), (1, 0)))
    l_k.wait()
    r_k.wait_recv()

    nblk = D // NC

    def wait_parts(group, first):
        for slot in range(first, 3):
            recv = remote(obuf.at[0], land.at[group, slot], os_sem.at[0], or_sem.at[group, slot], ynbr)
            if slot:
                recv.wait_recv()
            else:
                pl.when(jnp.logical_not(is_worker))(recv.wait_recv)

    def merge(group):
        parts = [land[group, w] for w in range(3)] + [newo[group]]
        tops = [p[TOP] for p in parts]
        top = functools.reduce(jnp.maximum, tops)
        scales = [jnp.exp2((m - top) * SCALE) for m in tops]
        total = sum(s * p[NORM] for s, p in zip(scales, parts))
        mixed = sum(s * p[OUT] for s, p in zip(scales, parts)) / total
        turned = mixed.T.astype(BF16)
        return jnp.concatenate([turned[block(h, ROWS)] for h in range(HEADS)], axis=1)

    def w_copy(e, i):
        piece = asend.at[i, pl.ds(pl.multiple_of(e * ROWS, ROWS), ROWS)]
        return remote(piece, arecv.at[i], ws_sem.at[e, i], wr_sem.at[i], {'cp': x * 2 + e, 'tp': to})

    def wait_new():
        for dc in range(1, 4):
            src = lax.rem(c + dc, 4)
            remote(kvbuf.at[src], kvbuf.at[src], kvs_sem.at[0], kvr_sem.at[src], ynbr).wait_recv()

    def new_rows(group, query, dev):
        keys = jnp.concatenate([kvbuf[b, 0] for b in range(4)], axis=0)
        vals = jnp.concatenate([kvbuf[b, 1] for b in range(4)], axis=0)
        key_pos = rel_position(lax.broadcasted_iota(jnp.int32, (256, QT), 0))
        lane = lax.broadcasted_iota(jnp.int32, (1, QT), 1) & (ROWS - 1)
        scores = lax.dot_general(keys, query, CONTRACT_LAST, preferred_element_type=F32)
        scores = jnp.where(key_pos <= rel_position(dev * ROWS + lane), scores, NEG)
        top = over_rows(jnp.max, scores)
        probs = jnp.exp2((scores - top) * SCALE)
        newo[group, OUT, :] = lax.dot_general(vals, probs.astype(BF16), (((0,), (0,)), ((), ())), preferred_element_type=F32)
        newo[group, TOP, :] = top
        newo[group, NORM, :] = over_rows(jnp.sum, probs)

    def tile_place(n):
        ph, i = lax.div(n, 4), lax.rem(n, 4)
        flip = par(jnp.maximum(ph, par(k, t)), lax.div(i, 2))
        dk = par(ph, i)
        blk = par(x, flip) * 2 + par(k, dk)
        j = par(k, 1, ph)
        return ph, blk, j, flip

    def o_copy(n):
        ph, blk, _, flip = tile_place(n)
        group = jnp.where(ph == 1, 2, par(blk))
        slot = jnp.where(is_worker, flip, 2)
        dev = jnp.where(ph == 1, blk, lax.div(blk, 2) * 2 + k)
        return remote(obuf.at[n + 1], land.at[group, slot], os_sem.at[n], or_sem.at[group, slot], {'cp': dev, 'tp': k})

    def stays(n):
        ph, blk, _, flip = tile_place(n)
        return jnp.logical_and(is_worker, jnp.where(ph == 1, blk == c, flip == 0))

    def goes(n):
        return jnp.logical_and(is_worker, jnp.logical_not(stays(n)))

    def far_copy(n):
        spot = lax.div(n, 4) * 2 + par(n)
        return remote(obuf.at[n + 1], passing.at[spot], os_sem.at[n], ps_sem.at[spot], {'cp': xo * 2 + k, 'tp': t})

    def wait_query(n):
        @pl.when(jnp.logical_not(jnp.logical_and(is_worker, lax.rem(n, 7) == 0)))
        def _():
            remote(qown.at[0], qbuf.at[n, :, :HEAD_DIM], qs_sem.at[0], qr_sem.at[n], ynbr).wait_recv()

    def part_rows(part):
        return slice(part * PART, (part + 1) * PART)

    def part_slots(ci, part):
        return slice(ci * CS + part * PART, ci * CS + (part + 1) * PART)

    def scores_of(qa, ci, part, top, s_ref):
        rows = part_slots(ci, part)
        ka = jnp.concatenate([kbuf[rows, :], vbuf[rows, :]], axis=1)
        s = lax.dot_general(ka, qa, CONTRACT_LAST, preferred_element_type=F32)
        s_ref[part_rows(part), :] = s
        mx = jnp.max(s.reshape(PART // 8, 8, QT), axis=0)
        return mx if top is None else jnp.maximum(top, mx)

    def probs_of(part, m, l, s_ref, p_ref):
        p = jnp.exp2((s_ref[part_rows(part), :] - m) * SCALE)
        p_ref[part_rows(part), :] = p.astype(BF16)
        return l + jnp.sum(p.reshape(PART // 8, 8, QT), axis=0)

    def values_of(ci, part, acc, p_ref):
        prod = jnp.dot(vt[:, part_slots(ci, part)], p_ref[part_rows(part), :], preferred_element_type=F32)
        return prod if acc is None else acc + prod

    def send_out(n):
        ph, blk, _, flip = tile_place(n)

        @pl.when(stays(n))
        def _():
            land[jnp.where(ph == 1, 2, par(blk)), 0] = obuf[n + 1]

        @pl.when(goes(n))
        def _():
            o_copy(n).start()

        @pl.when(jnp.logical_not(is_worker))
        def _():
            @pl.when(flip == 1)
            def _():
                far_copy(n).start()

            @pl.when(flip == 0)
            def _():
                spot = ph * 2 + par(n)
                far_copy(n).wait_recv()
                both = (obuf[n + 1], passing[spot])
                tops = [p[TOP] for p in both]
                top = jnp.maximum(tops[0], tops[1])
                scales = [jnp.exp2((m - top) * SCALE) for m in tops]
                obuf[n + 1, OUT, :] = scales[0] * both[0][OUT] + scales[1] * both[1][OUT]
                obuf[n + 1, TOP, :] = top
                obuf[n + 1, NORM, :] = scales[0] * both[0][NORM] + scales[1] * both[1][NORM]
                o_copy(n).start()

    sp = ((s0, p0), (s1, p1))
    nparts = CS // PART

    def chunk(state, ci, query):
        m, l, tops, alphas = state
        s_ref, p_ref = sp[ci % 2]
        m_new = tops[0] if ci == 0 else jnp.maximum(m, tops[0])
        alpha_new = jnp.exp2((m - m_new) * SCALE) if ci else jnp.zeros((1, QT), F32)
        l = l * alpha_new
        nxt = acc = None
        for part in range(nparts):
            if alphas is not None:
                acc = values_of((ci - 2) % NCH, part, acc, p_ref)
            l = probs_of(part, m_new, l, s_ref, p_ref)
            if query is not None:
                nxt = scores_of(query, (ci + 2) % NCH, part, nxt, s_ref)
        tops = (tops[1], tops[1] if nxt is None else over_rows(jnp.max, nxt))
        if alphas is None:
            return m_new, l, tops, alpha_new
        oacc[...] = oacc[...] * alphas[0] + acc
        return m_new, l, tops, (alphas[1], alpha_new)

    def put_stats(n, m, l):
        obuf[n + 1, TOP, :] = m
        obuf[n + 1, NORM, :] = over_rows(jnp.sum, l)

    def tile_step(n, carry):
        between(n)
        state = carry[0], carry[1], carry[2:4], carry[4:6]
        q_now, q_next = qbuf[n], qbuf[n + 1]
        for ci in range(2, NCH):
            state = chunk(state, ci, q_now if ci + 2 < NCH else q_next)
        put_stats(n, state[0], state[1])
        for ci in PAIR:
            state = chunk(state, ci, q_next)
        obuf[n + 1, OUT, :] = oacc[...]
        m, l, tops, alphas = state
        return (m, l) + tops + alphas

    def between(n):
        @pl.when(n > 0)
        def _():
            send_out(n - 1)

        @pl.when(n == 0)
        def _():
            send_queries(1, ((1, 1), (1, 0), (0, 1), (0, 0)))
            for dc in range(1, 4):
                kv_copy(dc).start()

        @pl.when(n == ASIDE - 1)
        def _():
            l_wo.wait()
            wait_new()
            for e in PAIR:
                pl.when(is_worker)(functools.partial(new_rows, e, qbuf[par(e, k), :, :HEAD_DIM], (x * 2 + e) * 2 + to))

        @pl.when(jnp.logical_and(n == ASIDE, is_worker))
        def _():
            def first_rows(order, _):
                e = par(k, order)
                wait_parts(e, 1)
                vals = merge(e)
                for i in range(nblk):
                    asend[i, pl.ds(pl.multiple_of(e * ROWS, ROWS), ROWS), :] = jnp.dot(vals, wo[:, block(i, NC)], preferred_element_type=F32)
                    w_copy(e, i).start()
                return 0

            lax.fori_loop(0, 2, first_rows, 0)

        @pl.when(n < 7)
        def _():
            wait_query(n + 1)

    wait_query(0)
    tops = []
    for ci in PAIR:
        top = None
        for part in range(nparts):
            top = scores_of(qbuf[0], ci, part, top, sp[ci][0])
        tops.append(over_rows(jnp.max, top))
    m, l, tops, alpha0 = chunk((None, jnp.zeros((8, QT), F32), tuple(tops), None), 0, qbuf[0])
    m, l, tops, alpha1 = chunk((m, l, tops, None), 1, qbuf[0])
    m, l, top0, top1, alpha0, alpha1 = lax.fori_loop(0, 7, tile_step, (m, l) + tops + (alpha0, alpha1))
    between(7)
    state = m, l, (top0, top1), (alpha0, alpha1)
    for ci in range(2, NCH):
        state = chunk(state, ci, qbuf[7] if ci + 2 < NCH else None)
    put_stats(7, state[0], state[1])
    for ci in PAIR:
        acc = None
        for part in range(nparts):
            acc = values_of(NCH - 2 + ci, part, acc, sp[ci][1])
        oacc[...] = oacc[...] * state[3][ci] + acc
    obuf[8, OUT, :] = oacc[...]
    send_out(7)

    new_rows(2, qown[t], c * 2 + t)
    wait_parts(2, 0)
    vals = merge(2)
    for i in range(nblk):
        hbuf[:, block(i, NC)] = jnp.dot(vals, wo[:, block(i, NC)], preferred_element_type=F32)
    l_g2.wait()
    for i in range(nblk):
        w_copy(0, i).wait_recv()
        cols = block(i, NC)
        hbuf[:, cols] = (x_ref[:, cols].astype(F32) + (hbuf[:, cols] + arecv[i])).astype(BF16).astype(F32)
    mid = hbuf[...]

    place = pl.multiple_of((k * 2 + t) * ROWS, ROWS)
    bbuf[pl.ds(place, ROWS), :] = rms(mid, wide(g2_ref))

    def b_copy(kind, i):
        rows = place if kind < 2 else pl.multiple_of((k * 2 + to) * ROWS, ROWS)
        piece = bbuf.at[pl.ds(rows, ROWS), i * KC:(i + 1) * KC]
        return remote(piece, piece, bs_sem.at[kind, i], br_sem.at[kind, i], partner if kind else ynbr)

    nk = D // KC
    for i in range(nk):
        b_copy(0, i).start()
        b_copy(1, i).start()
    def drain(n, _):
        _, _, _, flip = tile_place(n)
        far = jnp.logical_and(jnp.logical_not(is_worker), flip == 1)

        @pl.when(far)
        def _():
            far_copy(n).wait_send()

        @pl.when(jnp.logical_not(jnp.logical_or(far, stays(n))))
        def _():
            o_copy(n).wait_send()
        return 0

    lax.fori_loop(0, 8, drain, 0)

    @pl.when(is_worker)
    def _():
        for i in range(nblk):
            for e in PAIR:
                w_copy(e, i).wait_send()

    l_wg.wait()
    l_wu.wait()
    nf = FCOLS // 256

    def acc_ref(i):
        if i < 16:
            return (s0, s1)[i // 8].at[i % 8 * 128:(i % 8 + 1) * 128]
        return obuf.at[i - 16, :128]

    cuts = (0, 4, 8, nf)

    def u_copy(i):
        piece = ubuf.at[k, :, cuts[i] * 256:cuts[i + 1] * 256]
        return remote(piece, piece, us_sem.at[i], ur_sem.at[i], partner)

    def forward(i):
        b_copy(0, i).wait_recv()
        b_copy(2, i).start()

    forward(0)
    for i in range(nk):
        if i + 1 < nk:
            forward(i + 1)
        b_copy(1, i).wait_recv()
        b_copy(2, i).wait_recv()
        acts2 = bbuf[:, i * KC:(i + 1) * KC]
        for f in range(nf):
            cols = slice(f * 256, (f + 1) * 256)
            gate = jnp.dot(acts2, wg[i * KC:(i + 1) * KC, cols], preferred_element_type=F32)
            up = jnp.dot(acts2, wu[i * KC:(i + 1) * KC, cols], preferred_element_type=F32)
            if i:
                gate = gate + acc_ref(2 * f)[...]
                up = up + acc_ref(2 * f + 1)[...]
            if i + 1 < nk:
                acc_ref(2 * f)[...] = gate
                acc_ref(2 * f + 1)[...] = up
            else:
                vals = gate / (1.0 + jnp.exp(-gate)) * up
                if f == 0:
                    keep = lax.broadcasted_iota(jnp.int32, (4 * ROWS, 256), 1) >= k * (2 * FCOLS - 5504)
                    vals = jnp.where(keep, vals, 0.0)
                ubuf[k, :, cols] = vals.astype(BF16)
                if f + 1 in cuts:
                    u_copy(cuts.index(f + 1) - 1).start()
    l_wd.wait()

    def d_copy(n):
        piece = asend.at[n * 2 + ko, pl.ds(myrow, ROWS)]
        return remote(piece, drecv.at[n], ds_sem.at[n], dr_sem.at[n], partner)

    def y_copy(n, e):
        piece = asend.at[n * 2 + e, pl.ds(other_row, ROWS)]
        return remote(piece, yrecv.at[k, n], ys_sem.at[n, e], yr_sem.at[k, n], {'cp': x * 2 + e, 'tp': to})

    def down_of(core, n):
        rows = pl.ds(pl.multiple_of(core * (5504 - FCOLS), 128), FCOLS)
        return jnp.dot(ubuf[core], wd[rows, block(n, NC)], preferred_element_type=F32)

    other_row = pl.multiple_of(to * ROWS, ROWS)
    halves = range(nblk // 2)
    for n in halves:
        prod = down_of(k, n)
        for e in PAIR:
            asend[n * 2 + e] = prod[block(e, 64)]
    for i in range(3):
        u_copy(i).wait_recv()
    for n in halves:
        prod = down_of(ko, n)
        for e in PAIR:
            asend[n * 2 + e] = asend[n * 2 + e] + prod[block(e, 64)]
        for e in PAIR:
            y_copy(n, e).start()
        d_copy(n).start()

    def out_copy(core, n):
        cols = pl.ds(pl.multiple_of(core * (D // 2) + n * NC, NC), NC)
        return pltpu.make_async_copy(out_ref.at[:, cols], out_hbm.at[:, cols], out_sem.at[core, n])

    def finish(core, n, base):
        remote(yrecv.at[core, n], yrecv.at[core, n], ys_sem.at[n, 0], yr_sem.at[core, n], ynbr).wait_recv()
        cols = pl.ds(pl.multiple_of(core * (D // 2) + n * NC, NC), NC)
        out_ref[:, cols] = (hbuf[:, cols] + (base + yrecv[core, n])).astype(BF16)
        out_copy(core, n).start()

    for n in halves:
        finish(k, n, asend[n * 2 + k, pl.ds(myrow, ROWS), :])
        d_copy(n).wait_recv()
        finish(ko, n, drecv[n])

    for n in halves:
        for core in (k, ko):
            out_copy(core, n).wait()

    r_v.wait_send()
    r_k.wait_send()
    for ph in PAIR:
        for dx, dy in ((0, 1), (0, 0), (1, 0), (1, 1)):
            if dx or dy:
                q_copy(dx, dy, ph).wait_send()
            else:
                @pl.when(jnp.logical_not(is_worker))
                def _():
                    q_copy(0, 0, ph).wait_send()
    for dc in range(1, 4):
        kv_copy(dc).wait_send()

    for kind in range(3):
        for i in range(nk):
            b_copy(kind, i).wait_send()
    for i in range(3):
        u_copy(i).wait_send()
    for n in halves:
        d_copy(n).wait_send()
        for e in PAIR:
            y_copy(n, e).wait_send()


def solution(mesh):
    token_spec = P(('dp', 'cp', 'tp'), None)
    column_spec = P(None, 'tp')
    row_spec = P('tp', None)

    def device_layer(hidden_loc, pos_loc, cache_len, cache_k, cache_v, norm1_gain, w_query, w_key, w_value, w_out, norm2_gain, w_gate, w_up, w_down):
        inv_freq = 1.0 / (ROPE_BASE ** (jnp.arange(HEAD_DIM // 2, dtype=F32) * (2.0 / HEAD_DIM)))
        freq = jnp.broadcast_to(inv_freq[None, :], (8, HEAD_DIM // 2))
        hbm = pl.BlockSpec(memory_space=pl.ANY)
        dma = pltpu.SemaphoreType.DMA
        return pl.pallas_call(
            kernel,
            out_shape=jax.ShapeDtypeStruct((ROWS, D), BF16),
            in_specs=[pl.BlockSpec(memory_space=pltpu.SMEM)] + [hbm] * 13,
            out_specs=hbm,
            scratch_shapes=[
                pltpu.VMEM((ROWS, D), BF16), pltpu.VMEM((8, 64), F32), pltpu.VMEM((16, 128), BF16), pltpu.VMEM((16, 128), BF16),
                pltpu.VMEM((D, 1024), BF16), pltpu.VMEM((D, 128), BF16), pltpu.VMEM((D, 128), BF16), pltpu.VMEM((1024, D), BF16),
                pltpu.VMEM((D, FCOLS), BF16), pltpu.VMEM((D, FCOLS), BF16), pltpu.VMEM((5504, D // 2), BF16),
                pltpu.VMEM((SLOTS, HEAD_DIM), BF16), pltpu.VMEM((SLOTS, HEAD_DIM), BF16), pltpu.VMEM((HEAD_DIM, SLOTS), BF16),
                pltpu.VMEM((2 * ROWS, D), BF16), pltpu.VMEM((2, QT, HEAD_DIM), BF16), pltpu.VMEM((8, QT, 2 * HEAD_DIM), BF16),
                pltpu.VMEM((4, 2, 64, HEAD_DIM), BF16),
                pltpu.VMEM((CS, QT), F32), pltpu.VMEM((CS, QT), F32), pltpu.VMEM((CS, QT), BF16), pltpu.VMEM((CS, QT), BF16),
                pltpu.VMEM((HEAD_DIM, QT), F32),
                pltpu.VMEM((9, OROWS, QT), F32), pltpu.VMEM((4, OROWS, QT), F32), pltpu.VMEM((3, 3, OROWS, QT), F32), pltpu.VMEM((3, OROWS, QT), F32),
                pltpu.VMEM((ROWS, D), F32), pltpu.VMEM((D // NC, 2 * ROWS, NC), F32), pltpu.VMEM((D // NC, ROWS, NC), F32),
                pltpu.VMEM((4 * ROWS, D), BF16), pltpu.VMEM((2, 4 * ROWS, FCOLS), BF16),
                pltpu.VMEM((2, ROWS, NC), F32), pltpu.VMEM((2, 2, ROWS, NC), F32), pltpu.VMEM((ROWS, D), BF16),
                *(dma(shape) for shape in ((13,), (2,), (2,), (2,), (8,), (8,), (4,), (4,), (8,), (4,), (3, 3), (2, 4), (4,), (3, D // KC), (3, D // KC),
                                           (3,), (3,), (2,), (2,), (2, 2), (2, 2), (2, 2))),
            ],
            compiler_params=pltpu.CompilerParams(collective_id=0, has_side_effects=True, vmem_limit_bytes=67043328),
            name='layer',
        )(cache_len, hidden_loc, freq, norm1_gain.reshape(16, 128), norm2_gain.reshape(16, 128), cache_k, cache_v,
          w_query, w_key, w_value, w_out, w_gate, w_up, w_down)

    return jax.shard_map(device_layer, mesh=mesh, in_specs=(token_spec, P(('dp', 'cp', 'tp')), P('dp'), token_spec, token_spec, P(), column_spec, column_spec, column_spec, row_spec, P(), column_spec, column_spec, row_spec), out_specs=token_spec, check_vma=False)
```

```python
import functools
import itertools
import math
import operator

import jax
import jax.numpy as jnp
from jax import lax
from jax.experimental import pallas as pl
from jax.experimental.pallas import tpu as pltpu
from jax.sharding import PartitionSpec as P

HEAD_DIM = 128
ROPE_BASE = 500000.0
NORM_EPS = 1e-5
MESH = pl.DeviceIdType.MESH
F32 = jnp.float32
BF16 = jnp.bfloat16

ROWS = 32
D = 2048
HEADS = 8
SLOTS = 8192
HALF = 4096
QT = ROWS * HEADS
CS = 1024
NCH = SLOTS // CS
VT = 512
ASIDE = 5
KC = 512
NC = 512
PART = 512
FCOLS = 2816
NEG = -(2.0 ** 100)
SCALE = math.log2(math.e) / math.sqrt(HEAD_DIM)
OROWS = HEAD_DIM + 8
PAIR = range(2)
OUT, TOP, NORM = (slice(*b) for b in ((0, HEAD_DIM), (HEAD_DIM, HEAD_DIM + 1), (HEAD_DIM + 1, HEAD_DIM + 2)))
CONTRACT_LAST = (((1,), (1,)), ((), ()))
PI_A = 201.0 / 128.0
PI_B = round((math.pi / 2 - PI_A) * 2.0 ** 20) / 2.0 ** 20
PI_C = math.pi / 2 - PI_A - PI_B


def rel_position(index):
    half = ROWS // 2
    dev, high = index >> 5, (index >> 4) & 1
    seg = dev + high * (15 - 2 * dev)
    return seg * half + (index & (half - 1))


def turn(angle):
    n = jnp.floor(angle * (2.0 / math.pi) + 0.5)
    r = ((angle - n * PI_A) - n * PI_B) - n * PI_C
    z = r * r
    sin = r + r * z * (-1.6666654611e-1 + z * (8.3321608736e-3 + z * -1.9515295891e-4))
    cos = 1.0 - 0.5 * z + z * z * (4.166664568298827e-2 + z * (-1.388731625493765e-3 + z * 2.443315711809948e-5))
    quarter = n - 4.0 * jnp.floor(n * 0.25)
    odd = (quarter == 1.0) | (quarter == 3.0)
    cos, sin = jnp.where(odd, sin, cos), jnp.where(odd, cos, sin)
    return jnp.where((quarter == 1.0) | (quarter == 2.0), -cos, cos), jnp.where(quarter >= 2.0, -sin, sin)


def par(first, *more):
    return lax.rem(sum(more, first), 2)


def over_rows(op, vals):
    return op(vals, axis=0, keepdims=True)


def block(i, size):
    return slice(i * size, (i + 1) * size)


def wide(gain_ref):
    gain = gain_ref[...].astype(F32)
    return jnp.concatenate([gain[i:i + 1] for i in range(D // 128)], axis=1)


def rms(values, gain):
    inv = lax.rsqrt(jnp.mean(values * values, axis=-1, keepdims=True) + NORM_EPS)
    return (values * inv * gain).astype(BF16)


def kernel(len_ref, x_hbm, freq_hbm, g1_hbm, g2_hbm, ck_ref, cv_ref, wq_hbm, wk_hbm, wv_hbm, wo_hbm, wg_hbm, wu_hbm, wd_hbm,
           out_hbm,
           x_ref, freq_ref, g1_ref, g2_ref, wq, wk, wv, wo, wg, wu, wd, kbuf, vbuf, vt, abuf, qown, qbuf, kvbuf, s0, s1, p0, p1, oacc, obuf, passing, land, newo, hbuf, asend, arecv,
           bbuf, ubuf, drecv, yrecv, out_ref,
           ld_sem, cs_sem, cr_sem, as_sem, ar_sem, qs_sem, qr_sem, kvs_sem, kvr_sem, os_sem, ps_sem, or_sem, ws_sem, wr_sem, bs_sem, br_sem,
           us_sem, ur_sem, ds_sem, dr_sem, ys_sem, yr_sem, out_sem):
    c = lax.axis_index('cp')
    t = lax.axis_index('tp')
    x, k = lax.div(c, 2), par(c)
    xo, ko, to = 1 - x, 1 - k, 1 - t
    partner = {'cp': x * 2 + ko, 'tp': t}
    ynbr = {'cp': c, 'tp': to}
    is_worker = k == t

    def remote(src, dst, ssem, rsem, dev):
        return pltpu.make_async_remote_copy(src_ref=src, dst_ref=dst, send_sem=ssem, recv_sem=rsem, device_id=dev, device_id_type=MESH)

    barrier = pltpu.get_barrier_semaphore()
    for dc in range(4):
        for dt in PAIR:
            if dc or dt:
                pl.semaphore_signal(barrier, inc=1, device_id={'cp': lax.rem(c + dc, 4), 'tp': par(t, dt)}, device_id_type=MESH)

    def local(src, dst, i):
        return pltpu.make_async_copy(src, dst, ld_sem.at[i])

    kcol = pl.multiple_of(k * HEAD_DIM, HEAD_DIM)
    kocol = pl.multiple_of(ko * HEAD_DIM, HEAD_DIM)
    myhalf = pl.multiple_of(k * HALF, HALF)
    fcol = pl.multiple_of(k * (5504 - FCOLS), 128)
    l_wq = local(wq_hbm, wq, 0)
    l_wk = local(wk_hbm, wk, 1)
    l_wv = local(wv_hbm, wv, 2)
    l_k = local(ck_ref.at[:, pl.ds(kcol, HEAD_DIM)], kbuf.at[pl.ds(myhalf, HALF), :], 3)
    l_v = local(cv_ref.at[:, pl.ds(kcol, HEAD_DIM)], vbuf.at[pl.ds(myhalf, HALF), :], 4)
    l_wo = local(wo_hbm, wo, 5)
    l_wg = local(wg_hbm.at[:, pl.ds(fcol, FCOLS)], wg, 6)
    l_wu = local(wu_hbm.at[:, pl.ds(fcol, FCOLS)], wu, 7)
    l_wd = local(wd_hbm.at[:, pl.ds(pl.multiple_of(k * (D // 2), 128), D // 2)], wd, 8)
    l_x = local(x_hbm, x_ref, 9)
    l_g1 = local(g1_hbm, g1_ref, 10)
    l_g2 = local(g2_hbm, g2_ref, 11)
    l_freq = local(freq_hbm, freq_ref, 12)
    for copy in (l_x, l_g1, l_wq, l_v, l_wk, l_wv, l_freq, l_k, l_g2):
        copy.start()

    l_x.wait()
    l_g1.wait()
    g1 = wide(g1_ref)
    myrow = pl.multiple_of(t * ROWS, ROWS)
    abuf[pl.ds(myrow, ROWS), :] = rms(x_ref[...].astype(F32), g1)

    pl.semaphore_wait(barrier, 7)
    def a_copy(i):
        piece = abuf.at[pl.ds(myrow, ROWS), block(i, D // 2)]
        return remote(piece, piece, as_sem.at[i], ar_sem.at[i], ynbr)

    for i in PAIR:
        a_copy(i).start()
    r_v = remote(cv_ref.at[:, pl.ds(kocol, HEAD_DIM)], vbuf.at[pl.ds(myhalf, HALF), :], cs_sem.at[0], cr_sem.at[0], partner)
    r_k = remote(ck_ref.at[:, pl.ds(kocol, HEAD_DIM)], kbuf.at[pl.ds(myhalf, HALF), :], cs_sem.at[1], cr_sem.at[1], partner)
    r_v.start()
    r_k.start()

    clen = len_ref[0]
    rowi, lane = (lax.broadcasted_iota(jnp.int32, (VT, HEAD_DIM), i) for i in PAIR)
    lane0 = lane == 0
    eye = operator.eq(*(lax.broadcasted_iota(jnp.int32, (HEAD_DIM, HEAD_DIM), i) for i in PAIR)).astype(F32).astype(BF16)

    def turn_half(core):
        def body(i, _):
            off = pl.multiple_of(core * HALF + i * VT, VT)
            vals = vbuf[pl.ds(off, VT), :]
            vt[:, pl.ds(off, VT)] = lax.dot_general(eye, vals, CONTRACT_LAST, preferred_element_type=F32).astype(BF16)
            hidden = (rowi + (HALF * (4 * x + 2 * core + t) + i * VT) >= clen) & lane0
            vbuf[pl.ds(off, VT), :] = jnp.where(hidden, NEG, 0.0).astype(BF16)
            return 0
        lax.fori_loop(0, HALF // VT, body, 0)

    l_v.wait()
    turn_half(k)

    one_col = (lax.broadcasted_iota(jnp.int32, (QT, HEAD_DIM), 1) == 0).astype(F32).astype(BF16)
    for n in range(8):
        qbuf[n, :, HEAD_DIM:] = one_col
    l_freq.wait()
    pos = clen + rel_position(c * 64 + lax.broadcasted_iota(jnp.int32, (64, HEAD_DIM // 2), 0))
    cos, sin = turn(pos.astype(F32) * freq_ref[0:1, :])
    oacc[...] = jnp.zeros((HEAD_DIM, QT), F32)

    l_wq.wait()
    l_wk.wait()
    l_wv.wait()
    for copy in (l_wo, l_wg, l_wu, l_wd):
        copy.start()
    cos = jnp.concatenate([cos, cos], axis=1)
    sin = jnp.concatenate([-sin, sin], axis=1)

    def rope(vals):
        return (vals * cos + pltpu.roll(vals, HEAD_DIM // 2, 1) * sin).astype(BF16)

    def q_copy(dx, dy, ph, half):
        j = to if ph == 0 else t
        dev = {'cp': par(x, dx) * 2 + t, 'tp': par(t, dy)}
        n = (dx * 2 + dy) * 2 + ph
        tile = ph * 4 + (dx + max(dy, ph)) % 2 * 2 + par(k, t, ph)
        rows = block(half, QT // 2)
        return remote(qown.at[j, rows], qbuf.at[tile, rows, :HEAD_DIM], qs_sem.at[n, half], qr_sem.at[tile, half], dev)

    def send_queries(ph, places, half):
        for dx, dy in places:
            copy = q_copy(dx, dy, ph, half)
            if dx or dy:
                copy.start()
            else:
                pl.when(jnp.logical_not(is_worker))(copy.start)

    for i in PAIR:
        a_copy(i).wait()
        acts = abuf[:, block(i, D // 2)]
        for hp in range(HEADS // 2):
            prod = jnp.dot(acts, wq[block(i, D // 2), block(hp, 256)], preferred_element_type=F32)
            if i == 0:
                s0[block(hp, 64), :] = prod
                continue
            prod = prod + s0[block(hp, 64), :]
            for sub in PAIR:
                rot = rope(prod[:, block(sub, HEAD_DIM)])
                for j in PAIR:
                    qown[j, block(hp * 2 + sub, ROWS), :] = rot[block(j, ROWS)]
            if hp % 2:
                send_queries(0, ((1, 1), (0, 0)), hp // 2)


    @pl.when(is_worker)
    def _():
        qbuf[0, :, :HEAD_DIM] = qown[to]
        qbuf[7, :, :HEAD_DIM] = qown[t]

    acts = abuf[...]
    kvbuf[c, 0] = rope(jnp.dot(acts, wk[...], preferred_element_type=F32))
    kvbuf[c, 1] = jnp.dot(acts, wv[...], preferred_element_type=F32).astype(BF16)

    def kv_copy(dc):
        return remote(kvbuf.at[c], kvbuf.at[c], kvs_sem.at[dc], kvr_sem.at[c], {'cp': lax.rem(c + dc, 4), 'tp': t})

    r_v.wait_recv()
    turn_half(ko)
    for half in PAIR:
        send_queries(0, ((0, 1), (1, 0)), half)
    for dc in range(1, 4):
        kv_copy(dc).start()
    for half in PAIR:
        send_queries(1, ((1, 1), (1, 0), (0, 1), (0, 0)), half)
    l_k.wait()
    r_k.wait_recv()

    nblk = D // NC

    def wait_parts(group, first):
        for slot in range(first, 3):
            recv = remote(obuf.at[0], land.at[group, slot], os_sem.at[0], or_sem.at[group, slot], ynbr)
            if slot:
                recv.wait_recv()
            else:
                pl.when(jnp.logical_not(is_worker))(recv.wait_recv)

    def merge(group):
        parts = [land[group, w] for w in range(3)] + [newo[group]]
        tops = [p[TOP] for p in parts]
        top = functools.reduce(jnp.maximum, tops)
        scales = [jnp.exp2((m - top) * SCALE) for m in tops]
        total = sum(s * p[NORM] for s, p in zip(scales, parts))
        mixed = sum(s * p[OUT] for s, p in zip(scales, parts)) / total
        turned = mixed.T.astype(BF16)
        return jnp.concatenate([turned[block(h, ROWS)] for h in range(HEADS)], axis=1)

    def w_copy(e, i):
        piece = asend.at[i, pl.ds(pl.multiple_of(e * ROWS, ROWS), ROWS)]
        return remote(piece, arecv.at[i], ws_sem.at[e, i], wr_sem.at[i], {'cp': x * 2 + e, 'tp': to})

    def wait_new():
        for dc in range(1, 4):
            src = lax.rem(c + dc, 4)
            remote(kvbuf.at[src], kvbuf.at[src], kvs_sem.at[0], kvr_sem.at[src], ynbr).wait_recv()

    def new_rows(group, query, dev):
        keys = jnp.concatenate([kvbuf[b, 0] for b in range(4)], axis=0)
        vals = jnp.concatenate([kvbuf[b, 1] for b in range(4)], axis=0)
        key_pos = rel_position(lax.broadcasted_iota(jnp.int32, (256, QT), 0))
        lane = lax.broadcasted_iota(jnp.int32, (1, QT), 1) & (ROWS - 1)
        scores = lax.dot_general(keys, query, CONTRACT_LAST, preferred_element_type=F32)
        scores = jnp.where(key_pos <= rel_position(dev * ROWS + lane), scores, NEG)
        top = over_rows(jnp.max, scores)
        probs = jnp.exp2((scores - top) * SCALE)
        newo[group, OUT, :] = lax.dot_general(vals, probs.astype(BF16), (((0,), (0,)), ((), ())), preferred_element_type=F32)
        newo[group, TOP, :] = top
        newo[group, NORM, :] = over_rows(jnp.sum, probs)

    def tile_place(n):
        ph, i = lax.div(n, 4), lax.rem(n, 4)
        flip = par(jnp.maximum(ph, par(k, t)), lax.div(i, 2))
        dk = par(ph, i)
        blk = par(x, flip) * 2 + par(k, dk)
        j = par(k, 1, ph)
        return ph, blk, j, flip

    def o_copy(n):
        ph, blk, _, flip = tile_place(n)
        group = jnp.where(ph == 1, 2, par(blk))
        slot = jnp.where(is_worker, flip, 2)
        dev = jnp.where(ph == 1, blk, lax.div(blk, 2) * 2 + k)
        return remote(obuf.at[n + 1], land.at[group, slot], os_sem.at[n], or_sem.at[group, slot], {'cp': dev, 'tp': k})

    def stays(n):
        ph, blk, _, flip = tile_place(n)
        return jnp.logical_and(is_worker, jnp.where(ph == 1, blk == c, flip == 0))

    def goes(n):
        return jnp.logical_and(is_worker, jnp.logical_not(stays(n)))

    def far_copy(n):
        spot = lax.div(n, 4) * 2 + par(n)
        return remote(obuf.at[n + 1], passing.at[spot], os_sem.at[n], ps_sem.at[spot], {'cp': xo * 2 + k, 'tp': t})

    def wait_query(n):
        @pl.when(jnp.logical_not(jnp.logical_and(is_worker, lax.rem(n, 7) == 0)))
        def _():
            for half in PAIR:
                rows = block(half, QT // 2)
                remote(qown.at[0, rows], qbuf.at[n, rows, :HEAD_DIM], qs_sem.at[0, half], qr_sem.at[n, half], ynbr).wait_recv()

    def part_rows(part):
        return slice(part * PART, (part + 1) * PART)

    def part_slots(ci, part):
        return slice(ci * CS + part * PART, ci * CS + (part + 1) * PART)

    def scores_of(qa, ci, part, top, s_ref):
        rows = part_slots(ci, part)
        ka = jnp.concatenate([kbuf[rows, :], vbuf[rows, :]], axis=1)
        s = lax.dot_general(ka, qa, CONTRACT_LAST, preferred_element_type=F32)
        s_ref[part_rows(part), :] = s
        mx = jnp.max(s.reshape(PART // 8, 8, QT), axis=0)
        return mx if top is None else jnp.maximum(top, mx)

    def probs_of(part, m, l, s_ref, p_ref):
        p = jnp.exp2((s_ref[part_rows(part), :] - m) * SCALE)
        p_ref[part_rows(part), :] = p.astype(BF16)
        return l + jnp.sum(p.reshape(PART // 8, 8, QT), axis=0)

    def values_of(ci, part, acc, p_ref):
        prod = jnp.dot(vt[:, part_slots(ci, part)], p_ref[part_rows(part), :], preferred_element_type=F32)
        return prod if acc is None else acc + prod

    def send_out(n):
        ph, blk, _, flip = tile_place(n)

        @pl.when(stays(n))
        def _():
            land[jnp.where(ph == 1, 2, par(blk)), 0] = obuf[n + 1]

        @pl.when(goes(n))
        def _():
            o_copy(n).start()

        @pl.when(jnp.logical_not(is_worker))
        def _():
            @pl.when(flip == 1)
            def _():
                far_copy(n).start()

            @pl.when(flip == 0)
            def _():
                spot = ph * 2 + par(n)
                far_copy(n).wait_recv()
                both = (obuf[n + 1], passing[spot])
                tops = [p[TOP] for p in both]
                top = jnp.maximum(tops[0], tops[1])
                scales = [jnp.exp2((m - top) * SCALE) for m in tops]
                obuf[n + 1, OUT, :] = scales[0] * both[0][OUT] + scales[1] * both[1][OUT]
                obuf[n + 1, TOP, :] = top
                obuf[n + 1, NORM, :] = scales[0] * both[0][NORM] + scales[1] * both[1][NORM]
                o_copy(n).start()

    sp = ((s0, p0), (s1, p1))
    nparts = CS // PART

    def chunk(state, ci, query):
        m, l, tops, alphas = state
        s_ref, p_ref = sp[ci % 2]
        m_new = tops[0] if ci == 0 else jnp.maximum(m, tops[0])
        alpha_new = jnp.exp2((m - m_new) * SCALE) if ci else jnp.zeros((1, QT), F32)
        l = l * alpha_new
        nxt = acc = None
        for part in range(nparts):
            if alphas is not None:
                acc = values_of((ci - 2) % NCH, part, acc, p_ref)
            l = probs_of(part, m_new, l, s_ref, p_ref)
            if query is not None:
                nxt = scores_of(query, (ci + 2) % NCH, part, nxt, s_ref)
        tops = (tops[1], tops[1] if nxt is None else over_rows(jnp.max, nxt))
        if alphas is None:
            return m_new, l, tops, alpha_new
        oacc[...] = oacc[...] * alphas[0] + acc
        return m_new, l, tops, (alphas[1], alpha_new)

    def put_stats(n, m, l):
        obuf[n + 1, TOP, :] = m
        obuf[n + 1, NORM, :] = over_rows(jnp.sum, l)

    def tile_step(n, carry):
        between(n)
        state = carry[0], carry[1], carry[2:4], carry[4:6]
        q_now, q_next = qbuf[n], qbuf[n + 1]
        for ci in range(2, NCH):
            state = chunk(state, ci, q_now if ci + 2 < NCH else q_next)
        put_stats(n, state[0], state[1])
        for ci in PAIR:
            state = chunk(state, ci, q_next)
        obuf[n + 1, OUT, :] = oacc[...]
        m, l, tops, alphas = state
        return (m, l) + tops + alphas

    def between(n):
        @pl.when(n > 0)
        def _():
            send_out(n - 1)

        @pl.when(n == ASIDE - 1)
        def _():
            l_wo.wait()
            wait_new()
            for e in PAIR:
                pl.when(is_worker)(functools.partial(new_rows, e, qbuf[par(e, k), :, :HEAD_DIM], (x * 2 + e) * 2 + to))

        @pl.when(is_worker & (n >= ASIDE) & (n < ASIDE + 2))
        def _():
            e = par(k, n - ASIDE)
            wait_parts(e, 1)
            vals = merge(e)
            for i in range(nblk):
                asend[i, pl.ds(pl.multiple_of(e * ROWS, ROWS), ROWS), :] = jnp.dot(vals, wo[:, block(i, NC)], preferred_element_type=F32)
                w_copy(e, i).start()

        @pl.when(n < 7)
        def _():
            wait_query(n + 1)

    wait_query(0)
    tops = []
    for ci in PAIR:
        top = None
        for part in range(nparts):
            top = scores_of(qbuf[0], ci, part, top, sp[ci][0])
        tops.append(over_rows(jnp.max, top))
    m, l, tops, alpha0 = chunk((None, jnp.zeros((8, QT), F32), tuple(tops), None), 0, qbuf[0])
    m, l, tops, alpha1 = chunk((m, l, tops, None), 1, qbuf[0])
    m, l, top0, top1, alpha0, alpha1 = lax.fori_loop(0, 7, tile_step, (m, l) + tops + (alpha0, alpha1))
    between(7)
    state = m, l, (top0, top1), (alpha0, alpha1)
    for ci in range(2, NCH):
        state = chunk(state, ci, qbuf[7] if ci + 2 < NCH else None)
    put_stats(7, state[0], state[1])
    for ci in PAIR:
        acc = None
        for part in range(nparts):
            acc = values_of(NCH - 2 + ci, part, acc, sp[ci][1])
        oacc[...] = oacc[...] * state[3][ci] + acc
    obuf[8, OUT, :] = oacc[...]
    send_out(7)

    new_rows(2, qown[t], c * 2 + t)
    wait_parts(2, 0)
    vals = merge(2)
    for i in range(nblk):
        hbuf[:, block(i, NC)] = jnp.dot(vals, wo[:, block(i, NC)], preferred_element_type=F32)
    l_g2.wait()
    for i in range(nblk):
        w_copy(0, i).wait_recv()
        cols = block(i, NC)
        hbuf[:, cols] = (x_ref[:, cols].astype(F32) + (hbuf[:, cols] + arecv[i])).astype(BF16).astype(F32)
    mid = hbuf[...]

    place = pl.multiple_of((k * 2 + t) * ROWS, ROWS)
    bbuf[pl.ds(place, ROWS), :] = rms(mid, wide(g2_ref))

    def b_piece(rows, i):
        return bbuf.at[pl.ds(rows, ROWS), block(i, KC)]

    def b_copy(kind, i):
        rows = place if kind < 2 else pl.multiple_of((k * 2 + to) * ROWS, ROWS)
        piece = b_piece(rows, i)
        return remote(piece, piece, bs_sem.at[kind, i], br_sem.at[kind, i], partner if kind else ynbr)

    nk = D // KC
    b_direct = remote(b_piece(place, 0), b_piece(place, 0), bs_sem.at[2, 0], br_sem.at[2, 0], {'cp': x * 2 + ko, 'tp': to})
    for i in range(nk):
        b_copy(0, i).start()
        if i == 0:
            b_direct.start()
        b_copy(1, i).start()
    def drain(n, _):
        _, _, _, flip = tile_place(n)
        far = jnp.logical_and(jnp.logical_not(is_worker), flip == 1)

        @pl.when(far)
        def _():
            far_copy(n).wait_send()

        @pl.when(jnp.logical_not(jnp.logical_or(far, stays(n))))
        def _():
            o_copy(n).wait_send()
        return 0

    lax.fori_loop(0, 8, drain, 0)

    @pl.when(is_worker)
    def _():
        for i in range(nblk):
            for e in PAIR:
                w_copy(e, i).wait_send()

    l_wg.wait()
    l_wu.wait()
    nf = FCOLS // 256

    def acc_ref(i):
        if i < 16:
            return (s0, s1)[i // 8].at[i % 8 * 128:(i % 8 + 1) * 128]
        return obuf.at[i - 16, :128]

    cuts = (0, 4, 8, nf)

    def u_copy(i):
        piece = ubuf.at[k, :, cuts[i] * 256:cuts[i + 1] * 256]
        return remote(piece, piece, us_sem.at[i], ur_sem.at[i], partner)

    def forward(i):
        b_copy(0, i).wait_recv()
        if i:
            b_copy(2, i).start()

    forward(0)
    for i in range(nk):
        if i + 1 < nk:
            forward(i + 1)
        b_copy(1, i).wait_recv()
        b_copy(2, i).wait_recv()
        acts2 = bbuf[:, i * KC:(i + 1) * KC]
        for f in range(nf):
            cols = slice(f * 256, (f + 1) * 256)
            gate = jnp.dot(acts2, wg[i * KC:(i + 1) * KC, cols], preferred_element_type=F32)
            up = jnp.dot(acts2, wu[i * KC:(i + 1) * KC, cols], preferred_element_type=F32)
            if i:
                gate = gate + acc_ref(2 * f)[...]
                up = up + acc_ref(2 * f + 1)[...]
            if i + 1 < nk:
                acc_ref(2 * f)[...] = gate
                acc_ref(2 * f + 1)[...] = up
            else:
                vals = gate / (1.0 + jnp.exp2(gate * -math.log2(math.e))) * up
                if f == 0:
                    keep = lax.broadcasted_iota(jnp.int32, (4 * ROWS, 256), 1) >= k * (2 * FCOLS - 5504)
                    vals = jnp.where(keep, vals, 0.0)
                ubuf[k, :, cols] = vals.astype(BF16)
                if f + 1 in cuts:
                    u_copy(cuts.index(f + 1) - 1).start()
    l_wd.wait()

    def d_copy(n):
        piece = asend.at[n * 2 + ko, pl.ds(myrow, ROWS)]
        return remote(piece, drecv.at[n], ds_sem.at[n], dr_sem.at[n], partner)

    def y_copy(n, e):
        piece = asend.at[n * 2 + e, pl.ds(other_row, ROWS)]
        return remote(piece, yrecv.at[k, n], ys_sem.at[n, e], yr_sem.at[k, n], {'cp': x * 2 + e, 'tp': to})

    def down_of(core, n):
        rows = pl.ds(pl.multiple_of(core * (5504 - FCOLS), 128), FCOLS)
        return jnp.dot(ubuf[core], wd[rows, block(n, NC)], preferred_element_type=F32)

    other_row = pl.multiple_of(to * ROWS, ROWS)
    halves = range(nblk // 2)
    for n in halves:
        prod = down_of(k, n)
        for e in PAIR:
            asend[n * 2 + e] = prod[block(e, 64)]
    for i in range(3):
        u_copy(i).wait_recv()
    for n in halves:
        prod = down_of(ko, n)
        for e in PAIR:
            asend[n * 2 + e] = asend[n * 2 + e] + prod[block(e, 64)]
        for e in PAIR:
            y_copy(n, e).start()
        d_copy(n).start()

    def out_copy(core, n):
        cols = pl.ds(pl.multiple_of(core * (D // 2) + n * NC, NC), NC)
        return pltpu.make_async_copy(out_ref.at[:, cols], out_hbm.at[:, cols], out_sem.at[core, n])

    def finish(core, n, base):
        remote(yrecv.at[core, n], yrecv.at[core, n], ys_sem.at[n, 0], yr_sem.at[core, n], ynbr).wait_recv()
        cols = pl.ds(pl.multiple_of(core * (D // 2) + n * NC, NC), NC)
        out_ref[:, cols] = (hbuf[:, cols] + (base + yrecv[core, n])).astype(BF16)
        out_copy(core, n).start()

    for n in halves:
        finish(k, n, asend[n * 2 + k, pl.ds(myrow, ROWS), :])
        d_copy(n).wait_recv()
        finish(ko, n, drecv[n])

    for n in halves:
        for core in (k, ko):
            out_copy(core, n).wait()

    r_v.wait_send()
    r_k.wait_send()
    for half in PAIR:
        for ph, dx, dy in itertools.product(PAIR, PAIR, PAIR):
            copy = q_copy(dx, dy, ph, half)
            if dx or dy:
                copy.wait_send()
            else:
                pl.when(jnp.logical_not(is_worker))(copy.wait_send)
    for dc in range(1, 4):
        kv_copy(dc).wait_send()

    for kind in range(3):
        for i in range(nk):
            b_copy(kind, i).wait_send()
    for i in range(3):
        u_copy(i).wait_send()
    for n in halves:
        d_copy(n).wait_send()
        for e in PAIR:
            y_copy(n, e).wait_send()


def solution(mesh):
    token_spec = P(('dp', 'cp', 'tp'), None)
    column_spec = P(None, 'tp')
    row_spec = P('tp', None)

    def device_layer(hidden_loc, pos_loc, cache_len, cache_k, cache_v, norm1_gain, w_query, w_key, w_value, w_out, norm2_gain, w_gate, w_up, w_down):
        inv_freq = 1.0 / (ROPE_BASE ** (jnp.arange(HEAD_DIM // 2, dtype=F32) * (2.0 / HEAD_DIM)))
        freq = jnp.broadcast_to(inv_freq[None, :], (8, HEAD_DIM // 2))
        hbm = pl.BlockSpec(memory_space=pl.ANY)
        dma = pltpu.SemaphoreType.DMA
        return pl.pallas_call(
            kernel,
            out_shape=jax.ShapeDtypeStruct((ROWS, D), BF16),
            in_specs=[pl.BlockSpec(memory_space=pltpu.SMEM)] + [hbm] * 13,
            out_specs=hbm,
            scratch_shapes=[
                pltpu.VMEM((ROWS, D), BF16), pltpu.VMEM((8, 64), F32), pltpu.VMEM((16, 128), BF16), pltpu.VMEM((16, 128), BF16),
                pltpu.VMEM((D, 1024), BF16), pltpu.VMEM((D, 128), BF16), pltpu.VMEM((D, 128), BF16), pltpu.VMEM((1024, D), BF16),
                pltpu.VMEM((D, FCOLS), BF16), pltpu.VMEM((D, FCOLS), BF16), pltpu.VMEM((5504, D // 2), BF16),
                pltpu.VMEM((SLOTS, HEAD_DIM), BF16), pltpu.VMEM((SLOTS, HEAD_DIM), BF16), pltpu.VMEM((HEAD_DIM, SLOTS), BF16),
                pltpu.VMEM((2 * ROWS, D), BF16), pltpu.VMEM((2, QT, HEAD_DIM), BF16), pltpu.VMEM((8, QT, 2 * HEAD_DIM), BF16),
                pltpu.VMEM((4, 2, 64, HEAD_DIM), BF16),
                pltpu.VMEM((CS, QT), F32), pltpu.VMEM((CS, QT), F32), pltpu.VMEM((CS, QT), BF16), pltpu.VMEM((CS, QT), BF16),
                pltpu.VMEM((HEAD_DIM, QT), F32),
                pltpu.VMEM((9, OROWS, QT), F32), pltpu.VMEM((4, OROWS, QT), F32), pltpu.VMEM((3, 3, OROWS, QT), F32), pltpu.VMEM((3, OROWS, QT), F32),
                pltpu.VMEM((ROWS, D), F32), pltpu.VMEM((D // NC, 2 * ROWS, NC), F32), pltpu.VMEM((D // NC, ROWS, NC), F32),
                pltpu.VMEM((4 * ROWS, D), BF16), pltpu.VMEM((2, 4 * ROWS, FCOLS), BF16),
                pltpu.VMEM((2, ROWS, NC), F32), pltpu.VMEM((2, 2, ROWS, NC), F32), pltpu.VMEM((ROWS, D), BF16),
                *(dma(shape) for shape in ((13,), (2,), (2,), (2,), (2,), (8, 2), (8, 2), (4,), (4,), (8,), (4,), (3, 3), (2, 4), (4,), (3, D // KC), (3, D // KC),
                                           (3,), (3,), (2,), (2,), (2, 2), (2, 2), (2, 2))),
            ],
            compiler_params=pltpu.CompilerParams(collective_id=0, has_side_effects=True, vmem_limit_bytes=67043328),
            name='layer',
        )(cache_len, hidden_loc, freq, norm1_gain.reshape(16, 128), norm2_gain.reshape(16, 128), cache_k, cache_v,
          w_query, w_key, w_value, w_out, w_gate, w_up, w_down)

    return jax.shard_map(device_layer, mesh=mesh, in_specs=(token_spec, P(('dp', 'cp', 'tp')), P('dp'), token_spec, token_spec, P(), column_spec, column_spec, column_spec, row_spec, P(), column_spec, column_spec, row_spec), out_specs=token_spec, check_vma=False)
```

```python
import functools
import itertools
import math
import operator

import jax
import jax.numpy as jnp
from jax import lax
from jax.experimental import pallas as pl
from jax.experimental.pallas import tpu as pltpu
from jax.sharding import PartitionSpec as P

HEAD_DIM = 128
ROPE_BASE = 500000.0
NORM_EPS = 1e-5
MESH = pl.DeviceIdType.MESH
F32 = jnp.float32
BF16 = jnp.bfloat16

ROWS = 32
D = 2048
HEADS = 8
SLOTS = 8192
HALF = 4096
QT = ROWS * HEADS
CS = 1024
NCH = SLOTS // CS
VT = 512
ASIDE = 5
KC = 512
NC = 512
PART = 512
FCOLS = 2816
NEG = -(2.0 ** 100)
SCALE = math.log2(math.e) / math.sqrt(HEAD_DIM)
OROWS = HEAD_DIM + 8
PAIR = range(2)
OUT, TOP, NORM = (slice(*b) for b in ((0, HEAD_DIM), (HEAD_DIM, HEAD_DIM + 1), (HEAD_DIM + 1, HEAD_DIM + 2)))
CONTRACT_LAST = (((1,), (1,)), ((), ()))
FREQ = 2 * math.log2(ROPE_BASE) / HEAD_DIM
FREQ_A = round(FREQ * 2 ** 16) / 2 ** 16
FREQ_B = FREQ - FREQ_A
PI_A = 201.0 / 128.0
PI_B = round((math.pi / 2 - PI_A) * 2.0 ** 20) / 2.0 ** 20
PI_C = math.pi / 2 - PI_A - PI_B


def rel_position(index):
    half = ROWS // 2
    dev, high = index >> 5, (index >> 4) & 1
    seg = dev + high * (15 - 2 * dev)
    return seg * half + (index & (half - 1))


def frequencies():
    lane = lax.broadcasted_iota(jnp.int32, (8, HEAD_DIM // 2), 1).astype(F32)
    whole = lane * FREQ_A
    n = jnp.floor(whole + 0.5)
    power = ((n - whole) - lane * FREQ_B) * math.log(2)
    series = 1.0
    for d in range(8, 0, -1):
        series = 1.0 + power * (1 / d) * series
    return series * jnp.exp2(-n)


def turn(angle):
    n = jnp.floor(angle * (2.0 / math.pi) + 0.5)
    r = ((angle - n * PI_A) - n * PI_B) - n * PI_C
    z = r * r
    sin = r + r * z * (-1.6666654611e-1 + z * (8.3321608736e-3 + z * -1.9515295891e-4))
    cos = 1.0 - 0.5 * z + z * z * (4.166664568298827e-2 + z * (-1.388731625493765e-3 + z * 2.443315711809948e-5))
    quarter = n - 4.0 * jnp.floor(n * 0.25)
    odd = (quarter == 1.0) | (quarter == 3.0)
    cos, sin = jnp.where(odd, sin, cos), jnp.where(odd, cos, sin)
    return jnp.where((quarter == 1.0) | (quarter == 2.0), -cos, cos), jnp.where(quarter >= 2.0, -sin, sin)


def par(first, *more):
    return lax.rem(sum(more, first), 2)


def over_rows(op, vals):
    return op(vals, axis=0, keepdims=True)


def block(i, size):
    return slice(i * size, (i + 1) * size)


def wide(gain_ref):
    gain = gain_ref[...].astype(F32)
    return jnp.concatenate([gain[i:i + 1] for i in range(D // 128)], axis=1)


def rms(values, gain):
    inv = lax.rsqrt(jnp.mean(values * values, axis=-1, keepdims=True) + NORM_EPS)
    return (values * inv * gain).astype(BF16)


def kernel(len_ref, x_hbm, g1_hbm, g2_hbm, ck_ref, cv_ref, wq_hbm, wk_hbm, wv_hbm, wo_hbm, wg_hbm, wu_hbm, wd_hbm,
           out_hbm,
           x_ref, g1_ref, g2_ref, wq, wk, wv, wo, wg, wu, wd, kbuf, vbuf, vt, abuf, qown, qbuf, kvbuf, s0, s1, p0, p1, oacc, obuf, passing, land, newo, hbuf, asend, arecv,
           bbuf, ubuf, drecv, yrecv, out_ref,
           ld_sem, cs_sem, cr_sem, as_sem, ar_sem, qs_sem, qr_sem, kvs_sem, kvr_sem, os_sem, ps_sem, or_sem, ws_sem, wr_sem, bs_sem, br_sem,
           us_sem, ur_sem, ds_sem, dr_sem, ys_sem, yr_sem, out_sem):
    c = lax.axis_index('cp')
    t = lax.axis_index('tp')
    x, k = lax.div(c, 2), par(c)
    xo, ko, to = 1 - x, 1 - k, 1 - t
    partner = {'cp': x * 2 + ko, 'tp': t}
    ynbr = {'cp': c, 'tp': to}
    is_worker = k == t

    def remote(src, dst, ssem, rsem, dev):
        return pltpu.make_async_remote_copy(src_ref=src, dst_ref=dst, send_sem=ssem, recv_sem=rsem, device_id=dev, device_id_type=MESH)

    barrier = pltpu.get_barrier_semaphore()
    for dc in range(4):
        for dt in PAIR:
            if dc or dt:
                pl.semaphore_signal(barrier, inc=1, device_id={'cp': lax.rem(c + dc, 4), 'tp': par(t, dt)}, device_id_type=MESH)

    def local(src, dst, i):
        return pltpu.make_async_copy(src, dst, ld_sem.at[i])

    kcol = pl.multiple_of(k * HEAD_DIM, HEAD_DIM)
    kocol = pl.multiple_of(ko * HEAD_DIM, HEAD_DIM)
    myhalf = pl.multiple_of(k * HALF, HALF)
    fcol = pl.multiple_of(k * (5504 - FCOLS), 128)
    l_wq = local(wq_hbm, wq, 0)
    l_wk = local(wk_hbm, wk, 1)
    l_wv = local(wv_hbm, wv, 2)
    l_k = local(ck_ref.at[:, pl.ds(kcol, HEAD_DIM)], kbuf.at[pl.ds(myhalf, HALF), :], 3)
    l_v = local(cv_ref.at[:, pl.ds(kcol, HEAD_DIM)], vbuf.at[pl.ds(myhalf, HALF), :], 4)
    l_wo = local(wo_hbm, wo, 5)
    l_wg = local(wg_hbm.at[:, pl.ds(fcol, FCOLS)], wg, 6)
    l_wu = local(wu_hbm.at[:, pl.ds(fcol, FCOLS)], wu, 7)
    l_wd = local(wd_hbm.at[:, pl.ds(pl.multiple_of(k * (D // 2), 128), D // 2)], wd, 8)
    l_x = local(x_hbm, x_ref, 9)
    l_g1 = local(g1_hbm, g1_ref, 10)
    l_g2 = local(g2_hbm, g2_ref, 11)
    for copy in (l_x, l_g1, l_wq, l_v, l_wk, l_wv, l_k, l_g2):
        copy.start()

    l_x.wait()
    l_g1.wait()
    g1 = wide(g1_ref)
    myrow = pl.multiple_of(t * ROWS, ROWS)
    abuf[pl.ds(myrow, ROWS), :] = rms(x_ref[...].astype(F32), g1)

    pl.semaphore_wait(barrier, 7)
    def a_copy(i):
        piece = abuf.at[pl.ds(myrow, ROWS), block(i, D // 2)]
        return remote(piece, piece, as_sem.at[i], ar_sem.at[i], ynbr)

    for i in PAIR:
        a_copy(i).start()
    r_v = remote(cv_ref.at[:, pl.ds(kocol, HEAD_DIM)], vbuf.at[pl.ds(myhalf, HALF), :], cs_sem.at[0], cr_sem.at[0], partner)
    r_k = remote(ck_ref.at[:, pl.ds(kocol, HEAD_DIM)], kbuf.at[pl.ds(myhalf, HALF), :], cs_sem.at[1], cr_sem.at[1], partner)
    r_v.start()
    r_k.start()

    clen = len_ref[0]
    rowi, lane = (lax.broadcasted_iota(jnp.int32, (VT, HEAD_DIM), i) for i in PAIR)
    lane0 = lane == 0
    eye = operator.eq(*(lax.broadcasted_iota(jnp.int32, (HEAD_DIM, HEAD_DIM), i) for i in PAIR)).astype(F32).astype(BF16)

    def turn_half(core):
        def body(i, _):
            off = pl.multiple_of(core * HALF + i * VT, VT)
            vals = vbuf[pl.ds(off, VT), :]
            vt[:, pl.ds(off, VT)] = lax.dot_general(eye, vals, CONTRACT_LAST, preferred_element_type=F32).astype(BF16)
            hidden = (rowi + (HALF * (4 * x + 2 * core + t) + i * VT) >= clen) & lane0
            vbuf[pl.ds(off, VT), :] = jnp.where(hidden, NEG, 0.0).astype(BF16)
            return 0
        lax.fori_loop(0, HALF // VT, body, 0)

    l_v.wait()
    turn_half(k)

    one_col = (lax.broadcasted_iota(jnp.int32, (QT, HEAD_DIM), 1) == 0).astype(F32).astype(BF16)
    for n in range(8):
        qbuf[n, :, HEAD_DIM:] = one_col
    pos = clen + rel_position(c * 64 + lax.broadcasted_iota(jnp.int32, (64, HEAD_DIM // 2), 0))
    cos, sin = turn(pos.astype(F32) * frequencies()[:1])
    oacc[...] = jnp.zeros((HEAD_DIM, QT), F32)

    l_wq.wait()
    l_wk.wait()
    l_wv.wait()
    for copy in (l_wo, l_wg, l_wu, l_wd):
        copy.start()
    cos = jnp.concatenate([cos, cos], axis=1)
    sin = jnp.concatenate([-sin, sin], axis=1)

    def rope(vals):
        return (vals * cos + pltpu.roll(vals, HEAD_DIM // 2, 1) * sin).astype(BF16)

    def q_copy(dx, dy, ph, half):
        j = to if ph == 0 else t
        dev = {'cp': par(x, dx) * 2 + t, 'tp': par(t, dy)}
        n = (dx * 2 + dy) * 2 + ph
        tile = ph * 4 + (dx + max(dy, ph)) % 2 * 2 + par(k, t, ph)
        rows = block(half, QT // 2)
        return remote(qown.at[j, rows], qbuf.at[tile, rows, :HEAD_DIM], qs_sem.at[n, half], qr_sem.at[tile, half], dev)

    def send_queries(ph, places, half):
        for dx, dy in places:
            copy = q_copy(dx, dy, ph, half)
            if dx or dy:
                copy.start()
            else:
                pl.when(jnp.logical_not(is_worker))(copy.start)

    for i in PAIR:
        a_copy(i).wait()
        acts = abuf[:, block(i, D // 2)]
        for hp in range(HEADS // 2):
            prod = jnp.dot(acts, wq[block(i, D // 2), block(hp, 256)], preferred_element_type=F32)
            if i == 0:
                s0[block(hp, 64), :] = prod
                continue
            prod = prod + s0[block(hp, 64), :]
            for sub in PAIR:
                rot = rope(prod[:, block(sub, HEAD_DIM)])
                for j in PAIR:
                    qown[j, block(hp * 2 + sub, ROWS), :] = rot[block(j, ROWS)]
            if hp % 2:
                send_queries(0, ((1, 1), (0, 0)), hp // 2)


    @pl.when(is_worker)
    def _():
        qbuf[0, :, :HEAD_DIM] = qown[to]
        qbuf[7, :, :HEAD_DIM] = qown[t]

    acts = abuf[...]
    kvbuf[c, 0] = rope(jnp.dot(acts, wk[...], preferred_element_type=F32))
    kvbuf[c, 1] = jnp.dot(acts, wv[...], preferred_element_type=F32).astype(BF16)

    def kv_copy(dc):
        return remote(kvbuf.at[c], kvbuf.at[c], kvs_sem.at[dc], kvr_sem.at[c], {'cp': lax.rem(c + dc, 4), 'tp': t})

    r_v.wait_recv()
    turn_half(ko)
    for half in PAIR:
        send_queries(0, ((0, 1), (1, 0)), half)
    for dc in range(1, 4):
        kv_copy(dc).start()
    for half in PAIR:
        send_queries(1, ((1, 1), (1, 0), (0, 1), (0, 0)), half)
    l_k.wait()
    r_k.wait_recv()

    nblk = D // NC

    def wait_parts(group, first):
        for slot in range(first, 3):
            recv = remote(obuf.at[0], land.at[group, slot], os_sem.at[0], or_sem.at[group, slot], ynbr)
            if slot:
                recv.wait_recv()
            else:
                pl.when(jnp.logical_not(is_worker))(recv.wait_recv)

    def merge(group):
        parts = [land[group, w] for w in range(3)] + [newo[group]]
        tops = [p[TOP] for p in parts]
        top = functools.reduce(jnp.maximum, tops)
        scales = [jnp.exp2((m - top) * SCALE) for m in tops]
        total = sum(s * p[NORM] for s, p in zip(scales, parts))
        mixed = sum(s * p[OUT] for s, p in zip(scales, parts)) / total
        turned = mixed.T.astype(BF16)
        return jnp.concatenate([turned[block(h, ROWS)] for h in range(HEADS)], axis=1)

    def w_copy(e, i):
        piece = asend.at[i, pl.ds(pl.multiple_of(e * ROWS, ROWS), ROWS)]
        return remote(piece, arecv.at[i], ws_sem.at[e, i], wr_sem.at[i], {'cp': x * 2 + e, 'tp': to})

    def wait_new():
        for dc in range(1, 4):
            src = lax.rem(c + dc, 4)
            remote(kvbuf.at[src], kvbuf.at[src], kvs_sem.at[0], kvr_sem.at[src], ynbr).wait_recv()

    def new_rows(group, query, dev):
        keys = jnp.concatenate([kvbuf[b, 0] for b in range(4)], axis=0)
        vals = jnp.concatenate([kvbuf[b, 1] for b in range(4)], axis=0)
        key_pos = rel_position(lax.broadcasted_iota(jnp.int32, (256, QT), 0))
        lane = lax.broadcasted_iota(jnp.int32, (1, QT), 1) & (ROWS - 1)
        scores = lax.dot_general(keys, query, CONTRACT_LAST, preferred_element_type=F32)
        scores = jnp.where(key_pos <= rel_position(dev * ROWS + lane), scores, NEG)
        top = over_rows(jnp.max, scores)
        probs = jnp.exp2((scores - top) * SCALE)
        newo[group, OUT, :] = lax.dot_general(vals, probs.astype(BF16), (((0,), (0,)), ((), ())), preferred_element_type=F32)
        newo[group, TOP, :] = top
        newo[group, NORM, :] = over_rows(jnp.sum, probs)

    def tile_place(n):
        ph, i = lax.div(n, 4), lax.rem(n, 4)
        flip = par(jnp.maximum(ph, par(k, t)), lax.div(i, 2))
        dk = par(ph, i)
        blk = par(x, flip) * 2 + par(k, dk)
        j = par(k, 1, ph)
        return ph, blk, j, flip

    def o_copy(n):
        ph, blk, _, flip = tile_place(n)
        group = jnp.where(ph == 1, 2, par(blk))
        slot = jnp.where(is_worker, flip, 2)
        dev = jnp.where(ph == 1, blk, lax.div(blk, 2) * 2 + k)
        return remote(obuf.at[n + 1], land.at[group, slot], os_sem.at[n], or_sem.at[group, slot], {'cp': dev, 'tp': k})

    def stays(n):
        ph, blk, _, flip = tile_place(n)
        return jnp.logical_and(is_worker, jnp.where(ph == 1, blk == c, flip == 0))

    def goes(n):
        return jnp.logical_and(is_worker, jnp.logical_not(stays(n)))

    def far_copy(n):
        spot = lax.div(n, 4) * 2 + par(n)
        return remote(obuf.at[n + 1], passing.at[spot], os_sem.at[n], ps_sem.at[spot], {'cp': xo * 2 + k, 'tp': t})

    def wait_query(n):
        @pl.when(jnp.logical_not(jnp.logical_and(is_worker, lax.rem(n, 7) == 0)))
        def _():
            for half in PAIR:
                rows = block(half, QT // 2)
                remote(qown.at[0, rows], qbuf.at[n, rows, :HEAD_DIM], qs_sem.at[0, half], qr_sem.at[n, half], ynbr).wait_recv()

    def part_rows(part):
        return slice(part * PART, (part + 1) * PART)

    def part_slots(ci, part):
        return slice(ci * CS + part * PART, ci * CS + (part + 1) * PART)

    def scores_of(qa, ci, part, top, s_ref):
        rows = part_slots(ci, part)
        ka = jnp.concatenate([kbuf[rows, :], vbuf[rows, :]], axis=1)
        s = lax.dot_general(ka, qa, CONTRACT_LAST, preferred_element_type=F32)
        s_ref[part_rows(part), :] = s
        mx = jnp.max(s.reshape(PART // 8, 8, QT), axis=0)
        return mx if top is None else jnp.maximum(top, mx)

    def probs_of(part, m, l, s_ref, p_ref):
        p = jnp.exp2((s_ref[part_rows(part), :] - m) * SCALE)
        p_ref[part_rows(part), :] = p.astype(BF16)
        return l + jnp.sum(p.reshape(PART // 8, 8, QT), axis=0)

    def values_of(ci, part, acc, p_ref):
        prod = jnp.dot(vt[:, part_slots(ci, part)], p_ref[part_rows(part), :], preferred_element_type=F32)
        return prod if acc is None else acc + prod

    def send_out(n):
        ph, blk, _, flip = tile_place(n)

        @pl.when(stays(n))
        def _():
            land[jnp.where(ph == 1, 2, par(blk)), 0] = obuf[n + 1]

        @pl.when(goes(n))
        def _():
            o_copy(n).start()

        @pl.when(jnp.logical_not(is_worker))
        def _():
            @pl.when(flip == 1)
            def _():
                far_copy(n).start()

            @pl.when(flip == 0)
            def _():
                spot = ph * 2 + par(n)
                far_copy(n).wait_recv()
                both = (obuf[n + 1], passing[spot])
                tops = [p[TOP] for p in both]
                top = jnp.maximum(tops[0], tops[1])
                scales = [jnp.exp2((m - top) * SCALE) for m in tops]
                obuf[n + 1, OUT, :] = scales[0] * both[0][OUT] + scales[1] * both[1][OUT]
                obuf[n + 1, TOP, :] = top
                obuf[n + 1, NORM, :] = scales[0] * both[0][NORM] + scales[1] * both[1][NORM]
                o_copy(n).start()

    sp = ((s0, p0), (s1, p1))
    nparts = CS // PART

    def chunk(state, ci, query):
        m, l, tops, alphas = state
        s_ref, p_ref = sp[ci % 2]
        m_new = tops[0] if ci == 0 else jnp.maximum(m, tops[0])
        alpha_new = jnp.exp2((m - m_new) * SCALE) if ci else jnp.zeros((1, QT), F32)
        l = l * alpha_new
        nxt = acc = None
        for part in range(nparts):
            if alphas is not None:
                acc = values_of((ci - 2) % NCH, part, acc, p_ref)
            l = probs_of(part, m_new, l, s_ref, p_ref)
            if query is not None:
                nxt = scores_of(query, (ci + 2) % NCH, part, nxt, s_ref)
        tops = (tops[1], tops[1] if nxt is None else over_rows(jnp.max, nxt))
        if alphas is None:
            return m_new, l, tops, alpha_new
        oacc[...] = oacc[...] * alphas[0] + acc
        return m_new, l, tops, (alphas[1], alpha_new)

    def put_stats(n, m, l):
        obuf[n + 1, TOP, :] = m
        obuf[n + 1, NORM, :] = over_rows(jnp.sum, l)

    def tile_step(n, carry):
        between(n)
        state = carry[0], carry[1], carry[2:4], carry[4:6]
        q_now, q_next = qbuf[n], qbuf[n + 1]
        for ci in range(2, NCH):
            state = chunk(state, ci, q_now if ci + 2 < NCH else q_next)
        put_stats(n, state[0], state[1])
        for ci in PAIR:
            state = chunk(state, ci, q_next)
        obuf[n + 1, OUT, :] = oacc[...]
        m, l, tops, alphas = state
        return (m, l) + tops + alphas

    def between(n):
        @pl.when(n > 0)
        def _():
            send_out(n - 1)

        @pl.when(n == ASIDE - 1)
        def _():
            l_wo.wait()
            wait_new()
            for e in PAIR:
                pl.when(is_worker)(functools.partial(new_rows, e, qbuf[par(e, k), :, :HEAD_DIM], (x * 2 + e) * 2 + to))

        @pl.when(is_worker & (n >= ASIDE) & (n < ASIDE + 2))
        def _():
            e = par(k, n - ASIDE)
            wait_parts(e, 1)
            vals = merge(e)
            for i in range(nblk):
                asend[i, pl.ds(pl.multiple_of(e * ROWS, ROWS), ROWS), :] = jnp.dot(vals, wo[:, block(i, NC)], preferred_element_type=F32)
                w_copy(e, i).start()

        @pl.when(n < 7)
        def _():
            wait_query(n + 1)

    wait_query(0)
    tops = []
    for ci in PAIR:
        top = None
        for part in range(nparts):
            top = scores_of(qbuf[0], ci, part, top, sp[ci][0])
        tops.append(over_rows(jnp.max, top))
    m, l, tops, alpha0 = chunk((None, jnp.zeros((8, QT), F32), tuple(tops), None), 0, qbuf[0])
    m, l, tops, alpha1 = chunk((m, l, tops, None), 1, qbuf[0])
    m, l, top0, top1, alpha0, alpha1 = lax.fori_loop(0, 7, tile_step, (m, l) + tops + (alpha0, alpha1))
    between(7)
    state = m, l, (top0, top1), (alpha0, alpha1)
    for ci in range(2, NCH):
        state = chunk(state, ci, qbuf[7] if ci + 2 < NCH else None)
    put_stats(7, state[0], state[1])
    for ci in PAIR:
        acc = None
        for part in range(nparts):
            acc = values_of(NCH - 2 + ci, part, acc, sp[ci][1])
        oacc[...] = oacc[...] * state[3][ci] + acc
    obuf[8, OUT, :] = oacc[...]
    send_out(7)

    new_rows(2, qown[t], c * 2 + t)
    wait_parts(2, 0)
    vals = merge(2)
    for i in range(nblk):
        hbuf[:, block(i, NC)] = jnp.dot(vals, wo[:, block(i, NC)], preferred_element_type=F32)
    l_g2.wait()
    for i in range(nblk):
        w_copy(0, i).wait_recv()
        cols = block(i, NC)
        hbuf[:, cols] = (x_ref[:, cols].astype(F32) + (hbuf[:, cols] + arecv[i])).astype(BF16).astype(F32)
    mid = hbuf[...]

    place = pl.multiple_of((k * 2 + t) * ROWS, ROWS)
    bbuf[pl.ds(place, ROWS), :] = rms(mid, wide(g2_ref))

    def b_piece(rows, i):
        return bbuf.at[pl.ds(rows, ROWS), block(i, KC)]

    def b_copy(kind, i):
        rows = place if kind < 2 else pl.multiple_of((k * 2 + to) * ROWS, ROWS)
        piece = b_piece(rows, i)
        return remote(piece, piece, bs_sem.at[kind, i], br_sem.at[kind, i], partner if kind else ynbr)

    nk = D // KC
    b_direct = remote(b_piece(place, 0), b_piece(place, 0), bs_sem.at[2, 0], br_sem.at[2, 0], {'cp': x * 2 + ko, 'tp': to})
    for i in range(nk):
        b_copy(0, i).start()
        if i == 0:
            b_direct.start()
        b_copy(1, i).start()
    def drain(n, _):
        _, _, _, flip = tile_place(n)
        far = jnp.logical_and(jnp.logical_not(is_worker), flip == 1)

        @pl.when(far)
        def _():
            far_copy(n).wait_send()

        @pl.when(jnp.logical_not(jnp.logical_or(far, stays(n))))
        def _():
            o_copy(n).wait_send()
        return 0

    lax.fori_loop(0, 8, drain, 0)

    @pl.when(is_worker)
    def _():
        for i in range(nblk):
            for e in PAIR:
                w_copy(e, i).wait_send()

    l_wg.wait()
    l_wu.wait()
    nf = FCOLS // 256

    def acc_ref(i):
        if i < 16:
            return (s0, s1)[i // 8].at[i % 8 * 128:(i % 8 + 1) * 128]
        return obuf.at[i - 16, :128]

    cuts = (0, 4, 8, nf)

    def u_copy(i):
        piece = ubuf.at[k, :, cuts[i] * 256:cuts[i + 1] * 256]
        return remote(piece, piece, us_sem.at[i], ur_sem.at[i], partner)

    def forward(i):
        b_copy(0, i).wait_recv()
        if i:
            b_copy(2, i).start()

    forward(0)
    for i in range(nk):
        if i + 1 < nk:
            forward(i + 1)
        b_copy(1, i).wait_recv()
        b_copy(2, i).wait_recv()
        acts2 = bbuf[:, i * KC:(i + 1) * KC]
        for f in range(nf):
            cols = slice(f * 256, (f + 1) * 256)
            gate = jnp.dot(acts2, wg[i * KC:(i + 1) * KC, cols], preferred_element_type=F32)
            up = jnp.dot(acts2, wu[i * KC:(i + 1) * KC, cols], preferred_element_type=F32)
            if i:
                gate = gate + acc_ref(2 * f)[...]
                up = up + acc_ref(2 * f + 1)[...]
            if i + 1 < nk:
                acc_ref(2 * f)[...] = gate
                acc_ref(2 * f + 1)[...] = up
            else:
                vals = gate / (1.0 + jnp.exp2(gate * -math.log2(math.e))) * up
                if f == 0:
                    keep = lax.broadcasted_iota(jnp.int32, (4 * ROWS, 256), 1) >= k * (2 * FCOLS - 5504)
                    vals = jnp.where(keep, vals, 0.0)
                ubuf[k, :, cols] = vals.astype(BF16)
                if f + 1 in cuts:
                    u_copy(cuts.index(f + 1) - 1).start()
    l_wd.wait()

    def d_copy(n):
        piece = asend.at[n * 2 + ko, pl.ds(myrow, ROWS)]
        return remote(piece, drecv.at[n], ds_sem.at[n], dr_sem.at[n], partner)

    def y_copy(n, e):
        piece = asend.at[n * 2 + e, pl.ds(other_row, ROWS)]
        return remote(piece, yrecv.at[k, n], ys_sem.at[n, e], yr_sem.at[k, n], {'cp': x * 2 + e, 'tp': to})

    def down_of(core, n):
        rows = pl.ds(pl.multiple_of(core * (5504 - FCOLS), 128), FCOLS)
        return jnp.dot(ubuf[core], wd[rows, block(n, NC)], preferred_element_type=F32)

    other_row = pl.multiple_of(to * ROWS, ROWS)
    halves = range(nblk // 2)
    for n in halves:
        prod = down_of(k, n)
        for e in PAIR:
            asend[n * 2 + e] = prod[block(e, 64)]
    for i in range(3):
        u_copy(i).wait_recv()
    for n in halves:
        prod = down_of(ko, n)
        for e in PAIR:
            asend[n * 2 + e] = asend[n * 2 + e] + prod[block(e, 64)]
        for e in PAIR:
            y_copy(n, e).start()
        d_copy(n).start()

    def out_copy(core, n):
        cols = pl.ds(pl.multiple_of(core * (D // 2) + n * NC, NC), NC)
        return pltpu.make_async_copy(out_ref.at[:, cols], out_hbm.at[:, cols], out_sem.at[core, n])

    def finish(core, n, base):
        remote(yrecv.at[core, n], yrecv.at[core, n], ys_sem.at[n, 0], yr_sem.at[core, n], ynbr).wait_recv()
        cols = pl.ds(pl.multiple_of(core * (D // 2) + n * NC, NC), NC)
        out_ref[:, cols] = (hbuf[:, cols] + (base + yrecv[core, n])).astype(BF16)
        out_copy(core, n).start()

    for n in halves:
        finish(k, n, asend[n * 2 + k, pl.ds(myrow, ROWS), :])
        d_copy(n).wait_recv()
        finish(ko, n, drecv[n])

    for n in halves:
        for core in (k, ko):
            out_copy(core, n).wait()

    r_v.wait_send()
    r_k.wait_send()
    for half in PAIR:
        for ph, dx, dy in itertools.product(PAIR, PAIR, PAIR):
            copy = q_copy(dx, dy, ph, half)
            if dx or dy:
                copy.wait_send()
            else:
                pl.when(jnp.logical_not(is_worker))(copy.wait_send)
    for dc in range(1, 4):
        kv_copy(dc).wait_send()

    for kind in range(3):
        for i in range(nk):
            b_copy(kind, i).wait_send()
    for i in range(3):
        u_copy(i).wait_send()
    for n in halves:
        d_copy(n).wait_send()
        for e in PAIR:
            y_copy(n, e).wait_send()


def solution(mesh):
    token_spec = P(('dp', 'cp', 'tp'), None)
    column_spec = P(None, 'tp')
    row_spec = P('tp', None)

    def device_layer(hidden_loc, pos_loc, cache_len, cache_k, cache_v, norm1_gain, w_query, w_key, w_value, w_out, norm2_gain, w_gate, w_up, w_down):
        hbm = pl.BlockSpec(memory_space=pl.ANY)
        dma = pltpu.SemaphoreType.DMA
        return pl.pallas_call(
            kernel,
            out_shape=jax.ShapeDtypeStruct((ROWS, D), BF16),
            in_specs=[pl.BlockSpec(memory_space=pltpu.SMEM)] + [hbm] * 12,
            out_specs=hbm,
            scratch_shapes=[
                pltpu.VMEM((ROWS, D), BF16), pltpu.VMEM((16, 128), BF16), pltpu.VMEM((16, 128), BF16),
                pltpu.VMEM((D, 1024), BF16), pltpu.VMEM((D, 128), BF16), pltpu.VMEM((D, 128), BF16), pltpu.VMEM((1024, D), BF16),
                pltpu.VMEM((D, FCOLS), BF16), pltpu.VMEM((D, FCOLS), BF16), pltpu.VMEM((5504, D // 2), BF16),
                pltpu.VMEM((SLOTS, HEAD_DIM), BF16), pltpu.VMEM((SLOTS, HEAD_DIM), BF16), pltpu.VMEM((HEAD_DIM, SLOTS), BF16),
                pltpu.VMEM((2 * ROWS, D), BF16), pltpu.VMEM((2, QT, HEAD_DIM), BF16), pltpu.VMEM((8, QT, 2 * HEAD_DIM), BF16),
                pltpu.VMEM((4, 2, 64, HEAD_DIM), BF16),
                pltpu.VMEM((CS, QT), F32), pltpu.VMEM((CS, QT), F32), pltpu.VMEM((CS, QT), BF16), pltpu.VMEM((CS, QT), BF16),
                pltpu.VMEM((HEAD_DIM, QT), F32),
                pltpu.VMEM((9, OROWS, QT), F32), pltpu.VMEM((4, OROWS, QT), F32), pltpu.VMEM((3, 3, OROWS, QT), F32), pltpu.VMEM((3, OROWS, QT), F32),
                pltpu.VMEM((ROWS, D), F32), pltpu.VMEM((D // NC, 2 * ROWS, NC), F32), pltpu.VMEM((D // NC, ROWS, NC), F32),
                pltpu.VMEM((4 * ROWS, D), BF16), pltpu.VMEM((2, 4 * ROWS, FCOLS), BF16),
                pltpu.VMEM((2, ROWS, NC), F32), pltpu.VMEM((2, 2, ROWS, NC), F32), pltpu.VMEM((ROWS, D), BF16),
                *(dma(shape) for shape in ((13,), (2,), (2,), (2,), (2,), (8, 2), (8, 2), (4,), (4,), (8,), (4,), (3, 3), (2, 4), (4,), (3, D // KC), (3, D // KC),
                                           (3,), (3,), (2,), (2,), (2, 2), (2, 2), (2, 2))),
            ],
            compiler_params=pltpu.CompilerParams(collective_id=0, has_side_effects=True, vmem_limit_bytes=67043328),
            name='layer',
        )(cache_len, hidden_loc, norm1_gain.reshape(16, 128), norm2_gain.reshape(16, 128), cache_k, cache_v,
          w_query, w_key, w_value, w_out, w_gate, w_up, w_down)

    return jax.shard_map(device_layer, mesh=mesh, in_specs=(token_spec, P(('dp', 'cp', 'tp')), P('dp'), token_spec, token_spec, P(), column_spec, column_spec, column_spec, row_spec, P(), column_spec, column_spec, row_spec), out_specs=token_spec, check_vma=False)
```

```python
import functools
import itertools
import math
import operator

import jax
import jax.numpy as jnp
from jax import lax
from jax.experimental import pallas as pl
from jax.experimental.pallas import tpu as pltpu
from jax.sharding import PartitionSpec as P

HEAD_DIM = 128
ROPE_BASE = 500000.0
NORM_EPS = 1e-5
MESH = pl.DeviceIdType.MESH
F32 = jnp.float32
BF16 = jnp.bfloat16

ROWS = 32
D = 2048
HEADS = 8
SLOTS = 8192
HALF = 4096
QT = ROWS * HEADS
CS = 1024
NCH = SLOTS // CS
VT = 512
ASIDE = 5
KC = 512
NC = 512
PART = 512
FCOLS = 2816
NEG = -(2.0 ** 100)
SCALE = math.log2(math.e) / math.sqrt(HEAD_DIM)
OROWS = HEAD_DIM + 8
PAIR = range(2)
OUT, TOP, NORM = (slice(*b) for b in ((0, HEAD_DIM), (HEAD_DIM, HEAD_DIM + 1), (HEAD_DIM + 1, HEAD_DIM + 2)))
CONTRACT_LAST = (((1,), (1,)), ((), ()))
FREQ = 2 * math.log2(ROPE_BASE) / HEAD_DIM
FREQ_A = round(FREQ * 2 ** 16) / 2 ** 16
FREQ_B = FREQ - FREQ_A
PI_A = 201.0 / 128.0
PI_B = round((math.pi / 2 - PI_A) * 2.0 ** 20) / 2.0 ** 20
PI_C = math.pi / 2 - PI_A - PI_B


def rel_position(index):
    half = ROWS // 2
    dev, high = index >> 5, (index >> 4) & 1
    seg = dev + high * (15 - 2 * dev)
    return seg * half + (index & (half - 1))


def frequencies():
    lane = lax.broadcasted_iota(jnp.int32, (8, HEAD_DIM // 2), 1).astype(F32)
    whole = lane * FREQ_A
    n = jnp.floor(whole + 0.5)
    power = ((n - whole) - lane * FREQ_B) * math.log(2)
    series = 1.0
    for d in range(8, 0, -1):
        series = 1.0 + power * (1 / d) * series
    return series * jnp.exp2(-n)


def turn(angle):
    n = jnp.floor(angle * (2.0 / math.pi) + 0.5)
    r = ((angle - n * PI_A) - n * PI_B) - n * PI_C
    z = r * r
    sin = r + r * z * (-1.6666654611e-1 + z * (8.3321608736e-3 + z * -1.9515295891e-4))
    cos = 1.0 - 0.5 * z + z * z * (4.166664568298827e-2 + z * (-1.388731625493765e-3 + z * 2.443315711809948e-5))
    quarter = n - 4.0 * jnp.floor(n * 0.25)
    odd = (quarter == 1.0) | (quarter == 3.0)
    cos, sin = jnp.where(odd, sin, cos), jnp.where(odd, cos, sin)
    return jnp.where((quarter == 1.0) | (quarter == 2.0), -cos, cos), jnp.where(quarter >= 2.0, -sin, sin)


def par(first, *more):
    return lax.rem(sum(more, first), 2)


def over_rows(op, vals):
    return op(vals, axis=0, keepdims=True)


def block(i, size):
    return slice(i * size, (i + 1) * size)


def wide(gain_ref):
    gain = gain_ref[...].astype(F32)
    return jnp.concatenate([gain[i:i + 1] for i in range(D // 128)], axis=1)


def rms(values, gain):
    inv = lax.rsqrt(jnp.mean(values * values, axis=-1, keepdims=True) + NORM_EPS)
    return (values * inv * gain).astype(BF16)


def kernel(len_ref, x_hbm, g1_hbm, g2_hbm, ck_ref, cv_ref, wq_hbm, wk_hbm, wv_hbm, wo_hbm, wg_hbm, wu_hbm, wd_hbm,
           out_hbm,
           x_ref, g1_ref, g2_ref, wq, wk, wv, wo, wg, wu, wd, kbuf, vbuf, vt, abuf, qown, qbuf, kvbuf, s0, s1, p0, p1, oacc, obuf, passing, land, newo, hbuf, asend, arecv,
           bbuf, ubuf, drecv, yrecv, out_ref,
           ld_sem, cs_sem, cr_sem, as_sem, ar_sem, qs_sem, qr_sem, kvs_sem, kvr_sem, os_sem, ps_sem, or_sem, ws_sem, wr_sem, bs_sem, br_sem,
           us_sem, ur_sem, ds_sem, dr_sem, ys_sem, yr_sem, out_sem):
    c = lax.axis_index('cp')
    t = lax.axis_index('tp')
    x, k = lax.div(c, 2), par(c)
    xo, ko, to = 1 - x, 1 - k, 1 - t
    partner = {'cp': x * 2 + ko, 'tp': t}
    ynbr = {'cp': c, 'tp': to}
    is_worker = k == t

    def remote(src, dst, ssem, rsem, dev):
        return pltpu.make_async_remote_copy(src_ref=src, dst_ref=dst, send_sem=ssem, recv_sem=rsem, device_id=dev, device_id_type=MESH)

    barrier = pltpu.get_barrier_semaphore()
    for dc in range(4):
        for dt in PAIR:
            if dc or dt:
                pl.semaphore_signal(barrier, inc=1, device_id={'cp': lax.rem(c + dc, 4), 'tp': par(t, dt)}, device_id_type=MESH)

    def local(src, dst, i):
        return pltpu.make_async_copy(src, dst, ld_sem.at[i])

    kcol = pl.multiple_of(k * HEAD_DIM, HEAD_DIM)
    kocol = pl.multiple_of(ko * HEAD_DIM, HEAD_DIM)
    myhalf = pl.multiple_of(k * HALF, HALF)
    fcol = pl.multiple_of(k * (5504 - FCOLS), 128)
    l_wq = local(wq_hbm, wq, 0)
    l_wk = local(wk_hbm, wk, 1)
    l_wv = local(wv_hbm, wv, 2)
    l_k = local(ck_ref.at[:, pl.ds(kcol, HEAD_DIM)], kbuf.at[pl.ds(myhalf, HALF), :], 3)
    l_v = local(cv_ref.at[:, pl.ds(kcol, HEAD_DIM)], vbuf.at[pl.ds(myhalf, HALF), :], 4)
    l_wo = local(wo_hbm, wo, 5)
    l_wg = local(wg_hbm.at[:, pl.ds(fcol, FCOLS)], wg, 6)
    l_wu = local(wu_hbm.at[:, pl.ds(fcol, FCOLS)], wu, 7)
    l_wd = local(wd_hbm.at[:, pl.ds(pl.multiple_of(k * (D // 2), 128), D // 2)], wd, 8)
    l_x = local(x_hbm, x_ref, 9)
    l_g1 = local(g1_hbm, g1_ref, 10)
    l_g2 = local(g2_hbm, g2_ref, 11)
    for copy in (l_x, l_g1, l_v, l_k, l_wq, l_wk, l_wv, l_g2):
        copy.start()

    l_x.wait()
    l_g1.wait()
    g1 = wide(g1_ref)
    myrow = pl.multiple_of(t * ROWS, ROWS)
    abuf[pl.ds(myrow, ROWS), :] = rms(x_ref[...].astype(F32), g1)

    pl.semaphore_wait(barrier, 7)
    def a_copy(i):
        piece = abuf.at[pl.ds(myrow, ROWS), block(i, D // 2)]
        return remote(piece, piece, as_sem.at[i], ar_sem.at[i], ynbr)

    for i in PAIR:
        a_copy(i).start()
    r_v = remote(cv_ref.at[:, pl.ds(kocol, HEAD_DIM)], vbuf.at[pl.ds(myhalf, HALF), :], cs_sem.at[0], cr_sem.at[0], partner)
    r_k = remote(ck_ref.at[:, pl.ds(kocol, HEAD_DIM)], kbuf.at[pl.ds(myhalf, HALF), :], cs_sem.at[1], cr_sem.at[1], partner)
    r_v.start()
    r_k.start()

    clen = len_ref[0]
    rowi, lane = (lax.broadcasted_iota(jnp.int32, (VT, HEAD_DIM), i) for i in PAIR)
    lane0 = lane == 0
    eye = operator.eq(*(lax.broadcasted_iota(jnp.int32, (HEAD_DIM, HEAD_DIM), i) for i in PAIR)).astype(F32).astype(BF16)

    def turn_half(core):
        def body(i, _):
            off = pl.multiple_of(core * HALF + i * VT, VT)
            rows = pl.ds(off, VT)
            gone = rowi + (HALF * (4 * x + 2 * core + t) + i * VT) >= clen
            vals = jnp.where(gone, 0.0, vbuf[rows, :].astype(F32)).astype(BF16)
            kbuf[rows, :] = jnp.where(gone, 0.0, kbuf[rows, :].astype(F32)).astype(BF16)
            vt[:, pl.ds(off, VT)] = lax.dot_general(eye, vals, CONTRACT_LAST, preferred_element_type=F32).astype(BF16)
            vbuf[rows, :] = jnp.where(gone & lane0, NEG, 0.0).astype(BF16)
            return 0
        lax.fori_loop(0, HALF // VT, body, 0)

    l_v.wait()
    l_k.wait()
    turn_half(k)

    one_col = (lax.broadcasted_iota(jnp.int32, (QT, HEAD_DIM), 1) == 0).astype(F32).astype(BF16)
    for n in range(8):
        qbuf[n, :, HEAD_DIM:] = one_col
    pos = clen + rel_position(c * 64 + lax.broadcasted_iota(jnp.int32, (64, HEAD_DIM // 2), 0))
    cos, sin = turn(pos.astype(F32) * frequencies()[:1])
    oacc[...] = jnp.zeros((HEAD_DIM, QT), F32)

    l_wq.wait()
    l_wk.wait()
    l_wv.wait()
    for copy in (l_wo, l_wg, l_wu, l_wd):
        copy.start()
    cos = jnp.concatenate([cos, cos], axis=1)
    sin = jnp.concatenate([-sin, sin], axis=1)

    def rope(vals):
        return (vals * cos + pltpu.roll(vals, HEAD_DIM // 2, 1) * sin).astype(BF16)

    def q_copy(dx, dy, ph, half):
        j = to if ph == 0 else t
        dev = {'cp': par(x, dx) * 2 + t, 'tp': par(t, dy)}
        n = (dx * 2 + dy) * 2 + ph
        tile = ph * 4 + (dx + max(dy, ph)) % 2 * 2 + par(k, t, ph)
        rows = block(half, QT // 2)
        return remote(qown.at[j, rows], qbuf.at[tile, rows, :HEAD_DIM], qs_sem.at[n, half], qr_sem.at[tile, half], dev)

    def send_queries(ph, places, half):
        for dx, dy in places:
            copy = q_copy(dx, dy, ph, half)
            if dx or dy:
                copy.start()
            else:
                pl.when(jnp.logical_not(is_worker))(copy.start)

    for i in PAIR:
        a_copy(i).wait()
        acts = abuf[:, block(i, D // 2)]
        for hp in range(HEADS // 2):
            prod = jnp.dot(acts, wq[block(i, D // 2), block(hp, 256)], preferred_element_type=F32)
            if i == 0:
                s0[block(hp, 64), :] = prod
                continue
            prod = prod + s0[block(hp, 64), :]
            for sub in PAIR:
                rot = rope(prod[:, block(sub, HEAD_DIM)])
                for j in PAIR:
                    qown[j, block(hp * 2 + sub, ROWS), :] = rot[block(j, ROWS)]
            if hp % 2:
                send_queries(0, ((1, 1), (0, 0)), hp // 2)


    @pl.when(is_worker)
    def _():
        qbuf[0, :, :HEAD_DIM] = qown[to]
        qbuf[7, :, :HEAD_DIM] = qown[t]

    acts = abuf[...]
    kvbuf[c, 0] = rope(jnp.dot(acts, wk[...], preferred_element_type=F32))
    kvbuf[c, 1] = jnp.dot(acts, wv[...], preferred_element_type=F32).astype(BF16)

    def kv_copy(dc):
        return remote(kvbuf.at[c], kvbuf.at[c], kvs_sem.at[dc], kvr_sem.at[c], {'cp': lax.rem(c + dc, 4), 'tp': t})

    r_v.wait_recv()
    r_k.wait_recv()
    turn_half(ko)
    for half in PAIR:
        send_queries(0, ((0, 1), (1, 0)), half)
    for dc in range(1, 4):
        kv_copy(dc).start()
    for half in PAIR:
        send_queries(1, ((1, 1), (1, 0), (0, 1), (0, 0)), half)

    nblk = D // NC

    def wait_parts(group, first):
        for slot in range(first, 3):
            recv = remote(obuf.at[0], land.at[group, slot], os_sem.at[0], or_sem.at[group, slot], ynbr)
            if slot:
                recv.wait_recv()
            else:
                pl.when(jnp.logical_not(is_worker))(recv.wait_recv)

    def merge(group):
        parts = [land[group, w] for w in range(3)] + [newo[group]]
        tops = [p[TOP] for p in parts]
        top = functools.reduce(jnp.maximum, tops)
        scales = [jnp.exp2((m - top) * SCALE) for m in tops]
        total = sum(s * p[NORM] for s, p in zip(scales, parts))
        mixed = sum(s * p[OUT] for s, p in zip(scales, parts)) / total
        turned = mixed.T.astype(BF16)
        return jnp.concatenate([turned[block(h, ROWS)] for h in range(HEADS)], axis=1)

    def w_copy(e, i):
        piece = asend.at[i, pl.ds(pl.multiple_of(e * ROWS, ROWS), ROWS)]
        return remote(piece, arecv.at[i], ws_sem.at[e, i], wr_sem.at[i], {'cp': x * 2 + e, 'tp': to})

    def wait_new():
        for dc in range(1, 4):
            src = lax.rem(c + dc, 4)
            remote(kvbuf.at[src], kvbuf.at[src], kvs_sem.at[0], kvr_sem.at[src], ynbr).wait_recv()

    def new_rows(group, query, dev):
        keys = jnp.concatenate([kvbuf[b, 0] for b in range(4)], axis=0)
        vals = jnp.concatenate([kvbuf[b, 1] for b in range(4)], axis=0)
        key_pos = rel_position(lax.broadcasted_iota(jnp.int32, (256, QT), 0))
        lane = lax.broadcasted_iota(jnp.int32, (1, QT), 1) & (ROWS - 1)
        scores = lax.dot_general(keys, query, CONTRACT_LAST, preferred_element_type=F32)
        scores = jnp.where(key_pos <= rel_position(dev * ROWS + lane), scores, NEG)
        top = over_rows(jnp.max, scores)
        probs = jnp.exp2((scores - top) * SCALE)
        newo[group, OUT, :] = lax.dot_general(vals, probs.astype(BF16), (((0,), (0,)), ((), ())), preferred_element_type=F32)
        newo[group, TOP, :] = top
        newo[group, NORM, :] = over_rows(jnp.sum, probs)

    def tile_place(n):
        ph, i = lax.div(n, 4), lax.rem(n, 4)
        flip = par(jnp.maximum(ph, par(k, t)), lax.div(i, 2))
        dk = par(ph, i)
        blk = par(x, flip) * 2 + par(k, dk)
        j = par(k, 1, ph)
        return ph, blk, j, flip

    def o_copy(n):
        ph, blk, _, flip = tile_place(n)
        group = jnp.where(ph == 1, 2, par(blk))
        slot = jnp.where(is_worker, flip, 2)
        dev = jnp.where(ph == 1, blk, lax.div(blk, 2) * 2 + k)
        return remote(obuf.at[n + 1], land.at[group, slot], os_sem.at[n], or_sem.at[group, slot], {'cp': dev, 'tp': k})

    def stays(n):
        ph, blk, _, flip = tile_place(n)
        return jnp.logical_and(is_worker, jnp.where(ph == 1, blk == c, flip == 0))

    def goes(n):
        return jnp.logical_and(is_worker, jnp.logical_not(stays(n)))

    def far_copy(n):
        spot = lax.div(n, 4) * 2 + par(n)
        return remote(obuf.at[n + 1], passing.at[spot], os_sem.at[n], ps_sem.at[spot], {'cp': xo * 2 + k, 'tp': t})

    def wait_query(n):
        @pl.when(jnp.logical_not(jnp.logical_and(is_worker, lax.rem(n, 7) == 0)))
        def _():
            for half in PAIR:
                rows = block(half, QT // 2)
                remote(qown.at[0, rows], qbuf.at[n, rows, :HEAD_DIM], qs_sem.at[0, half], qr_sem.at[n, half], ynbr).wait_recv()

    def part_rows(part):
        return slice(part * PART, (part + 1) * PART)

    def part_slots(ci, part):
        return slice(ci * CS + part * PART, ci * CS + (part + 1) * PART)

    def scores_of(qa, ci, part, top, s_ref):
        rows = part_slots(ci, part)
        ka = jnp.concatenate([kbuf[rows, :], vbuf[rows, :]], axis=1)
        s = lax.dot_general(ka, qa, CONTRACT_LAST, preferred_element_type=F32)
        s_ref[part_rows(part), :] = s
        mx = jnp.max(s.reshape(PART // 8, 8, QT), axis=0)
        return mx if top is None else jnp.maximum(top, mx)

    def probs_of(part, m, l, s_ref, p_ref):
        p = jnp.exp2((s_ref[part_rows(part), :] - m) * SCALE)
        p_ref[part_rows(part), :] = p.astype(BF16)
        return l + jnp.sum(p.reshape(PART // 8, 8, QT), axis=0)

    def values_of(ci, part, acc, p_ref):
        prod = jnp.dot(vt[:, part_slots(ci, part)], p_ref[part_rows(part), :], preferred_element_type=F32)
        return prod if acc is None else acc + prod

    def send_out(n):
        ph, blk, _, flip = tile_place(n)

        @pl.when(stays(n))
        def _():
            land[jnp.where(ph == 1, 2, par(blk)), 0] = obuf[n + 1]

        @pl.when(goes(n))
        def _():
            o_copy(n).start()

        @pl.when(jnp.logical_not(is_worker))
        def _():
            @pl.when(flip == 1)
            def _():
                far_copy(n).start()

            @pl.when(flip == 0)
            def _():
                spot = ph * 2 + par(n)
                far_copy(n).wait_recv()
                both = (obuf[n + 1], passing[spot])
                tops = [p[TOP] for p in both]
                top = jnp.maximum(tops[0], tops[1])
                scales = [jnp.exp2((m - top) * SCALE) for m in tops]
                obuf[n + 1, OUT, :] = scales[0] * both[0][OUT] + scales[1] * both[1][OUT]
                obuf[n + 1, TOP, :] = top
                obuf[n + 1, NORM, :] = scales[0] * both[0][NORM] + scales[1] * both[1][NORM]
                o_copy(n).start()

    sp = ((s0, p0), (s1, p1))
    nparts = CS // PART

    def chunk(state, ci, query):
        m, l, tops, alphas = state
        s_ref, p_ref = sp[ci % 2]
        m_new = tops[0] if ci == 0 else jnp.maximum(m, tops[0])
        alpha_new = jnp.exp2((m - m_new) * SCALE) if ci else jnp.zeros((1, QT), F32)
        l = l * alpha_new
        nxt = acc = None
        for part in range(nparts):
            if alphas is not None:
                acc = values_of((ci - 2) % NCH, part, acc, p_ref)
            l = probs_of(part, m_new, l, s_ref, p_ref)
            if query is not None:
                nxt = scores_of(query, (ci + 2) % NCH, part, nxt, s_ref)
        tops = (tops[1], tops[1] if nxt is None else over_rows(jnp.max, nxt))
        if alphas is None:
            return m_new, l, tops, alpha_new
        oacc[...] = oacc[...] * alphas[0] + acc
        return m_new, l, tops, (alphas[1], alpha_new)

    def put_stats(n, m, l):
        obuf[n + 1, TOP, :] = m
        obuf[n + 1, NORM, :] = over_rows(jnp.sum, l)

    def tile_step(n, carry):
        between(n)
        state = carry[0], carry[1], carry[2:4], carry[4:6]
        q_now, q_next = qbuf[n], qbuf[n + 1]
        for ci in range(2, NCH):
            state = chunk(state, ci, q_now if ci + 2 < NCH else q_next)
        put_stats(n, state[0], state[1])
        for ci in PAIR:
            state = chunk(state, ci, q_next)
        obuf[n + 1, OUT, :] = oacc[...]
        m, l, tops, alphas = state
        return (m, l) + tops + alphas

    def between(n):
        @pl.when(n > 0)
        def _():
            send_out(n - 1)

        @pl.when(n == ASIDE - 1)
        def _():
            l_wo.wait()
            wait_new()
            for e in PAIR:
                pl.when(is_worker)(functools.partial(new_rows, e, qbuf[par(e, k), :, :HEAD_DIM], (x * 2 + e) * 2 + to))

        @pl.when(is_worker & (n >= ASIDE) & (n < ASIDE + 2))
        def _():
            e = par(k, n - ASIDE)
            wait_parts(e, 1)
            vals = merge(e)
            for i in range(nblk):
                asend[i, pl.ds(pl.multiple_of(e * ROWS, ROWS), ROWS), :] = jnp.dot(vals, wo[:, block(i, NC)], preferred_element_type=F32)
                w_copy(e, i).start()

        @pl.when(n < 7)
        def _():
            wait_query(n + 1)

    wait_query(0)
    tops = []
    for ci in PAIR:
        top = None
        for part in range(nparts):
            top = scores_of(qbuf[0], ci, part, top, sp[ci][0])
        tops.append(over_rows(jnp.max, top))
    m, l, tops, alpha0 = chunk((None, jnp.zeros((8, QT), F32), tuple(tops), None), 0, qbuf[0])
    m, l, tops, alpha1 = chunk((m, l, tops, None), 1, qbuf[0])
    m, l, top0, top1, alpha0, alpha1 = lax.fori_loop(0, 7, tile_step, (m, l) + tops + (alpha0, alpha1))
    between(7)
    state = m, l, (top0, top1), (alpha0, alpha1)
    for ci in range(2, NCH):
        state = chunk(state, ci, qbuf[7] if ci + 2 < NCH else None)
    put_stats(7, state[0], state[1])
    for ci in PAIR:
        acc = None
        for part in range(nparts):
            acc = values_of(NCH - 2 + ci, part, acc, sp[ci][1])
        oacc[...] = oacc[...] * state[3][ci] + acc
    obuf[8, OUT, :] = oacc[...]
    send_out(7)

    new_rows(2, qown[t], c * 2 + t)
    wait_parts(2, 0)
    vals = merge(2)
    for i in range(nblk):
        hbuf[:, block(i, NC)] = jnp.dot(vals, wo[:, block(i, NC)], preferred_element_type=F32)
    l_g2.wait()
    for i in range(nblk):
        w_copy(0, i).wait_recv()
        cols = block(i, NC)
        hbuf[:, cols] = (x_ref[:, cols].astype(F32) + (hbuf[:, cols] + arecv[i])).astype(BF16).astype(F32)
    mid = hbuf[...]

    place = pl.multiple_of((k * 2 + t) * ROWS, ROWS)
    bbuf[pl.ds(place, ROWS), :] = rms(mid, wide(g2_ref))

    def b_piece(rows, i):
        return bbuf.at[pl.ds(rows, ROWS), block(i, KC)]

    def b_copy(kind, i):
        rows = place if kind < 2 else pl.multiple_of((k * 2 + to) * ROWS, ROWS)
        piece = b_piece(rows, i)
        return remote(piece, piece, bs_sem.at[kind, i], br_sem.at[kind, i], partner if kind else ynbr)

    nk = D // KC
    b_direct = remote(b_piece(place, 0), b_piece(place, 0), bs_sem.at[2, 0], br_sem.at[2, 0], {'cp': x * 2 + ko, 'tp': to})
    for i in range(nk):
        b_copy(0, i).start()
        if i == 0:
            b_direct.start()
        b_copy(1, i).start()
    def drain(n, _):
        _, _, _, flip = tile_place(n)
        far = jnp.logical_and(jnp.logical_not(is_worker), flip == 1)

        @pl.when(far)
        def _():
            far_copy(n).wait_send()

        @pl.when(jnp.logical_not(jnp.logical_or(far, stays(n))))
        def _():
            o_copy(n).wait_send()
        return 0

    lax.fori_loop(0, 8, drain, 0)

    @pl.when(is_worker)
    def _():
        for i in range(nblk):
            for e in PAIR:
                w_copy(e, i).wait_send()

    l_wg.wait()
    l_wu.wait()
    nf = FCOLS // 256

    def acc_ref(i):
        if i < 16:
            return (s0, s1)[i // 8].at[i % 8 * 128:(i % 8 + 1) * 128]
        return obuf.at[i - 16, :128]

    cuts = (0, 5, 9, nf)

    def u_copy(i):
        piece = ubuf.at[k, :, cuts[i] * 256:cuts[i + 1] * 256]
        return remote(piece, piece, us_sem.at[i], ur_sem.at[i], partner)

    def forward(i):
        b_copy(0, i).wait_recv()
        if i:
            b_copy(2, i).start()

    forward(0)
    for i in range(nk):
        if i + 1 < nk:
            forward(i + 1)
        b_copy(1, i).wait_recv()
        b_copy(2, i).wait_recv()
        acts2 = bbuf[:, i * KC:(i + 1) * KC]
        for f in range(nf):
            cols = slice(f * 256, (f + 1) * 256)
            gate = jnp.dot(acts2, wg[i * KC:(i + 1) * KC, cols], preferred_element_type=F32)
            up = jnp.dot(acts2, wu[i * KC:(i + 1) * KC, cols], preferred_element_type=F32)
            if i:
                gate = gate + acc_ref(2 * f)[...]
                up = up + acc_ref(2 * f + 1)[...]
            if i + 1 < nk:
                acc_ref(2 * f)[...] = gate
                acc_ref(2 * f + 1)[...] = up
            else:
                vals = gate / (1.0 + jnp.exp2(gate * -math.log2(math.e))) * up
                if f == 0:
                    keep = lax.broadcasted_iota(jnp.int32, (4 * ROWS, 256), 1) >= k * (2 * FCOLS - 5504)
                    vals = jnp.where(keep, vals, 0.0)
                ubuf[k, :, cols] = vals.astype(BF16)
                if f + 1 in cuts:
                    u_copy(cuts.index(f + 1) - 1).start()
    l_wd.wait()

    def d_copy(n):
        piece = asend.at[n * 2 + ko, pl.ds(myrow, ROWS)]
        return remote(piece, drecv.at[n], ds_sem.at[n], dr_sem.at[n], partner)

    def y_copy(n, e):
        piece = asend.at[n * 2 + e, pl.ds(other_row, ROWS)]
        return remote(piece, yrecv.at[k, n], ys_sem.at[n, e], yr_sem.at[k, n], {'cp': x * 2 + e, 'tp': to})

    def down_of(core, n):
        rows = pl.ds(pl.multiple_of(core * (5504 - FCOLS), 128), FCOLS)
        return jnp.dot(ubuf[core], wd[rows, block(n, NC)], preferred_element_type=F32)

    other_row = pl.multiple_of(to * ROWS, ROWS)
    halves = range(nblk // 2)
    for n in halves:
        prod = down_of(k, n)
        for e in PAIR:
            asend[n * 2 + e] = prod[block(e, 64)]
    for i in range(3):
        u_copy(i).wait_recv()
    for n in halves:
        prod = down_of(ko, n)
        for e in PAIR:
            asend[n * 2 + e] = asend[n * 2 + e] + prod[block(e, 64)]
        for e in PAIR:
            y_copy(n, e).start()
        d_copy(n).start()

    def out_copy(core, n):
        cols = pl.ds(pl.multiple_of(core * (D // 2) + n * NC, NC), NC)
        return pltpu.make_async_copy(out_ref.at[:, cols], out_hbm.at[:, cols], out_sem.at[core, n])

    def finish(core, n, base):
        remote(yrecv.at[core, n], yrecv.at[core, n], ys_sem.at[n, 0], yr_sem.at[core, n], ynbr).wait_recv()
        cols = pl.ds(pl.multiple_of(core * (D // 2) + n * NC, NC), NC)
        out_ref[:, cols] = (hbuf[:, cols] + (base + yrecv[core, n])).astype(BF16)
        out_copy(core, n).start()

    for n in halves:
        finish(k, n, asend[n * 2 + k, pl.ds(myrow, ROWS), :])
        d_copy(n).wait_recv()
        finish(ko, n, drecv[n])

    for n in halves:
        for core in (k, ko):
            out_copy(core, n).wait()

    r_v.wait_send()
    r_k.wait_send()
    for half in PAIR:
        for ph, dx, dy in itertools.product(PAIR, PAIR, PAIR):
            copy = q_copy(dx, dy, ph, half)
            if dx or dy:
                copy.wait_send()
            else:
                pl.when(jnp.logical_not(is_worker))(copy.wait_send)
    for dc in range(1, 4):
        kv_copy(dc).wait_send()

    for kind in range(3):
        for i in range(nk):
            b_copy(kind, i).wait_send()
    for i in range(3):
        u_copy(i).wait_send()
    for n in halves:
        d_copy(n).wait_send()
        for e in PAIR:
            y_copy(n, e).wait_send()


def solution(mesh):
    token_spec = P(('dp', 'cp', 'tp'), None)
    column_spec = P(None, 'tp')
    row_spec = P('tp', None)

    def device_layer(hidden_loc, pos_loc, cache_len, cache_k, cache_v, norm1_gain, w_query, w_key, w_value, w_out, norm2_gain, w_gate, w_up, w_down):
        hbm = pl.BlockSpec(memory_space=pl.ANY)
        dma = pltpu.SemaphoreType.DMA
        return pl.pallas_call(
            kernel,
            out_shape=jax.ShapeDtypeStruct((ROWS, D), BF16),
            in_specs=[pl.BlockSpec(memory_space=pltpu.SMEM)] + [hbm] * 12,
            out_specs=hbm,
            scratch_shapes=[
                pltpu.VMEM((ROWS, D), BF16), pltpu.VMEM((16, 128), BF16), pltpu.VMEM((16, 128), BF16),
                pltpu.VMEM((D, 1024), BF16), pltpu.VMEM((D, 128), BF16), pltpu.VMEM((D, 128), BF16), pltpu.VMEM((1024, D), BF16),
                pltpu.VMEM((D, FCOLS), BF16), pltpu.VMEM((D, FCOLS), BF16), pltpu.VMEM((5504, D // 2), BF16),
                pltpu.VMEM((SLOTS, HEAD_DIM), BF16), pltpu.VMEM((SLOTS, HEAD_DIM), BF16), pltpu.VMEM((HEAD_DIM, SLOTS), BF16),
                pltpu.VMEM((2 * ROWS, D), BF16), pltpu.VMEM((2, QT, HEAD_DIM), BF16), pltpu.VMEM((8, QT, 2 * HEAD_DIM), BF16),
                pltpu.VMEM((4, 2, 64, HEAD_DIM), BF16),
                pltpu.VMEM((CS, QT), F32), pltpu.VMEM((CS, QT), F32), pltpu.VMEM((CS, QT), BF16), pltpu.VMEM((CS, QT), BF16),
                pltpu.VMEM((HEAD_DIM, QT), F32),
                pltpu.VMEM((9, OROWS, QT), F32), pltpu.VMEM((4, OROWS, QT), F32), pltpu.VMEM((3, 3, OROWS, QT), F32), pltpu.VMEM((3, OROWS, QT), F32),
                pltpu.VMEM((ROWS, D), F32), pltpu.VMEM((D // NC, 2 * ROWS, NC), F32), pltpu.VMEM((D // NC, ROWS, NC), F32),
                pltpu.VMEM((4 * ROWS, D), BF16), pltpu.VMEM((2, 4 * ROWS, FCOLS), BF16),
                pltpu.VMEM((2, ROWS, NC), F32), pltpu.VMEM((2, 2, ROWS, NC), F32), pltpu.VMEM((ROWS, D), BF16),
                *(dma(shape) for shape in ((13,), (2,), (2,), (2,), (2,), (8, 2), (8, 2), (4,), (4,), (8,), (4,), (3, 3), (2, 4), (4,), (3, D // KC), (3, D // KC),
                                           (3,), (3,), (2,), (2,), (2, 2), (2, 2), (2, 2))),
            ],
            compiler_params=pltpu.CompilerParams(collective_id=0, has_side_effects=True, vmem_limit_bytes=67043328),
            name='layer',
        )(cache_len, hidden_loc, norm1_gain.reshape(16, 128), norm2_gain.reshape(16, 128), cache_k, cache_v,
          w_query, w_key, w_value, w_out, w_gate, w_up, w_down)

    return jax.shard_map(device_layer, mesh=mesh, in_specs=(token_spec, P(('dp', 'cp', 'tp')), P('dp'), token_spec, token_spec, P(), column_spec, column_spec, column_spec, row_spec, P(), column_spec, column_spec, row_spec), out_specs=token_spec, check_vma=False)
```
